128 devices in a mesh: pp: 2 (over core), dp: 64 (over z, y, x).
Axes of the slice: x: 4, y: 4, z: 4, core: 2. Of those that a mesh axis runs over, the one named last changes fastest.
Arguments:
- act_in: bfloat16 [8, 64, 384, 512], P(None, 'dp')
- loss_seed: bfloat16 [8, 64, 384, 512], P(None, 'dp')
- w_qkv: bfloat16 [2, 512, 24, 64], P('pp', 'dp')
- w_proj: bfloat16 [2, 512, 512], P('pp', 'dp')
- w_up: bfloat16 [2, 512, 2048], P('pp', 'dp')
- w_down: bfloat16 [2, 2048, 512], P('pp', 'dp')
Outputs:
- output 1: float32 [2, 512, 24, 64], P('pp', 'dp')
- output 2: float32 [2, 512, 512], P('pp', 'dp')
- output 3: float32 [2, 512, 2048], P('pp', 'dp')
- output 4: float32 [2, 2048, 512], P('pp', 'dp')
- output 5: bfloat16 [8, 64, 384, 512], P(None, 'dp', 'pp')
All inputs are finite; a program needn't handle non-finite values.
Results may differ from the reference program's by a relative error of at most 0.02.
Values are sent between devices in bfloat16 or wider.
A program may use at most 1 GiB of HBM per device.

```python
import jax
import jax.numpy as jnp
from jax import lax

MICROBATCHES = 8
DP_SIZE = 64
BATCH_DEV = 1
SEQ_LEN = 384
D_MODEL = 512
NUM_HEADS = 8
TOTAL_LAYERS = 2

HEAD_DIM = D_MODEL // NUM_HEADS
ROWS_ALL = DP_SIZE * BATCH_DEV
NORM_EPS = 1e-6


def setup_inputs(seed: int = 0) -> dict:
    key_list = jax.random.split(jax.random.key(seed), 6)
    act_shape = (MICROBATCHES, ROWS_ALL, SEQ_LEN, D_MODEL)
    seed_scale = (MICROBATCHES * ROWS_ALL * SEQ_LEN) ** -0.5
    act_in = jax.random.normal(key_list[0], act_shape, jnp.float32).astype(jnp.bfloat16)
    loss_seed = (jax.random.normal(key_list[1], act_shape, jnp.float32) * seed_scale).astype(jnp.bfloat16)
    w_qkv = (jax.random.normal(key_list[2], (TOTAL_LAYERS, D_MODEL, 3 * NUM_HEADS, HEAD_DIM), jnp.float32) * D_MODEL ** -0.5).astype(jnp.bfloat16)
    w_proj = (jax.random.normal(key_list[3], (TOTAL_LAYERS, D_MODEL, D_MODEL), jnp.float32) * D_MODEL ** -0.5).astype(jnp.bfloat16)
    w_up = (jax.random.normal(key_list[4], (TOTAL_LAYERS, D_MODEL, 4 * D_MODEL), jnp.float32) * D_MODEL ** -0.5).astype(jnp.bfloat16)
    w_down = (jax.random.normal(key_list[5], (TOTAL_LAYERS, 4 * D_MODEL, D_MODEL), jnp.float32) * (4 * D_MODEL) ** -0.5).astype(jnp.bfloat16)
    return {'act_in': act_in, 'loss_seed': loss_seed, 'w_qkv': w_qkv, 'w_proj': w_proj, 'w_up': w_up, 'w_down': w_down}


def bf16_cast(values):
    return values.astype(jnp.bfloat16).astype(jnp.float32)


def rms_norm(hidden):
    return hidden * lax.rsqrt(jnp.mean(hidden * hidden, axis=-1, keepdims=True) + NORM_EPS)


def layer_apply(hidden, layer_w):
    w_qkv, w_proj, w_up, w_down = layer_w
    hid_f32 = hidden.astype(jnp.float32)
    normed = bf16_cast(rms_norm(hid_f32))
    qkv_act = bf16_cast(jnp.einsum('bsd,dnh->bsnh', normed, w_qkv))
    q_heads = qkv_act[:, :, :NUM_HEADS]
    k_heads = qkv_act[:, :, NUM_HEADS:2 * NUM_HEADS]
    v_heads = qkv_act[:, :, 2 * NUM_HEADS:]
    scores = jnp.einsum('bqnh,bknh->bnqk', q_heads, k_heads) * HEAD_DIM ** -0.5
    causal = jnp.arange(SEQ_LEN)[:, None] >= jnp.arange(SEQ_LEN)[None, :]
    prob_bf = bf16_cast(jax.nn.softmax(jnp.where(causal, scores, -1e30), axis=-1))
    attn_out = bf16_cast(jnp.einsum('bnqk,bknh->bqnh', prob_bf, v_heads))
    attn_flat = attn_out.reshape(hidden.shape)
    mid_f32 = bf16_cast(hid_f32 + jnp.einsum('bse,ed->bsd', attn_flat, w_proj))
    normed2 = bf16_cast(rms_norm(mid_f32))
    up_act = bf16_cast(jnp.einsum('bsd,df->bsf', normed2, w_up))
    gelu_out = bf16_cast(jax.nn.gelu(up_act, approximate=True))
    return (mid_f32 + jnp.einsum('bsf,fd->bsd', gelu_out, w_down)).astype(jnp.bfloat16)


def stack_apply(weight_set, hidden):
    def layer_step(hidden_now, layer_w):
        return layer_apply(hidden_now, layer_w), None
    final_out, _ = lax.scan(jax.checkpoint(layer_step), hidden, weight_set)
    return final_out


def reference(act_in, loss_seed, w_qkv, w_proj, w_up, w_down):
    weights = (w_qkv.astype(jnp.float32), w_proj.astype(jnp.float32), w_up.astype(jnp.float32), w_down.astype(jnp.float32))
    rows_in = act_in.reshape(MICROBATCHES * DP_SIZE, BATCH_DEV, SEQ_LEN, D_MODEL)
    rows_seed = loss_seed.reshape(MICROBATCHES * DP_SIZE, BATCH_DEV, SEQ_LEN, D_MODEL)

    def row_step(grad_sum, row_pair):
        hidden, cotangent = row_pair
        rows_out, pull_back = jax.vjp(lambda weight_set: stack_apply(weight_set, hidden), weights)
        row_grads = pull_back(cotangent)[0]
        return tuple(acc_part + grad_part for acc_part, grad_part in zip(grad_sum, row_grads)), rows_out

    zero_grads = tuple(jnp.zeros_like(w_full) for w_full in weights)
    grad_sum, outs_all = lax.scan(row_step, zero_grads, (rows_in, rows_seed))
    act_out = outs_all.reshape(MICROBATCHES, ROWS_ALL, SEQ_LEN, D_MODEL)
    return grad_sum[0], grad_sum[1], grad_sum[2], grad_sum[3], act_out
```

```python
import functools

import jax
import jax.numpy as jnp
from jax import lax
from jax.experimental import pallas as pl
from jax.experimental.pallas import tpu as pltpu
from jax.sharding import Mesh
from jax.sharding import PartitionSpec as P

NORM_EPS = 1e-6
BF = jnp.bfloat16
F32 = jnp.float32


def rms_norm(hidden):
    return hidden * lax.rsqrt(jnp.mean(hidden * hidden, axis=-1, keepdims=True) + NORM_EPS)


def gelu_tanh(pre_act):
    return jax.nn.gelu(pre_act, approximate=True)


def dot(a, b):
    return lax.dot_general(a, b, (((1,), (0,)), ((), ())), preferred_element_type=F32)


def dot_nt(a, b):
    return lax.dot_general(a, b, (((1,), (1,)), ((), ())), preferred_element_type=F32)


def dot_tn(a, b):
    return lax.dot_general(a, b, (((0,), (0,)), ((), ())), preferred_element_type=F32)


def softmax_rows(q, kh, scale):
    s = dot_nt(q, kh) * scale
    row = lax.broadcasted_iota(jnp.int32, s.shape, 0)
    col = lax.broadcasted_iota(jnp.int32, s.shape, 1)
    s = jnp.where(row >= col, s, -1e30)
    e = jnp.exp(s - jnp.max(s, axis=-1, keepdims=True))
    return e * (1.0 / jnp.sum(e, axis=-1, keepdims=True))


def attn_fwd_kernel(scale, q_ref, k_ref, v_ref, o_ref):
    q, k, v = q_ref[...], k_ref[...], v_ref[...]
    low = lax.broadcasted_iota(jnp.int32, k.shape, 1) < 64
    zero = jnp.zeros_like(k)
    out = jnp.zeros(q.shape, F32)
    for half in range(2):
        keep = low if half == 0 else jnp.logical_not(low)
        p = softmax_rows(q, jnp.where(keep, k, zero), scale).astype(BF)
        out = out + dot(p, jnp.where(keep, v, zero))
    o_ref[...] = out.astype(BF)


def attn_bwd_kernel(scale, width, q_ref, k_ref, v_ref, do_ref, dqkv_ref):
    q, k, v, do = q_ref[...], k_ref[...], v_ref[...], do_ref[...]
    low = lax.broadcasted_iota(jnp.int32, k.shape, 1) < 64
    zero = jnp.zeros_like(k)
    dq = jnp.zeros(q.shape, F32)
    dk = jnp.zeros(q.shape, F32)
    dv = jnp.zeros(q.shape, F32)
    for half in range(2):
        keep = low if half == 0 else jnp.logical_not(low)
        kh, vh = jnp.where(keep, k, zero), jnp.where(keep, v, zero)
        qh, doh = jnp.where(keep, q, zero), jnp.where(keep, do, zero)
        p = softmax_rows(q, kh, scale)
        dp = dot_nt(do, vh).astype(BF).astype(F32)
        delta = jnp.sum(dp * p, axis=-1, keepdims=True)
        ds = (p * (dp - delta) * scale).astype(BF)
        dq = dq + dot(ds, kh)
        dk = dk + dot_tn(ds, qh)
        dv = dv + dot_tn(p.astype(BF), doh)
    base = pl.program_id(1) * 128
    dqkv_ref[:, pl.ds(pl.multiple_of(base, 128), 128)] = dq.astype(BF)
    dqkv_ref[:, pl.ds(pl.multiple_of(base + width, 128), 128)] = dk.astype(BF)
    dqkv_ref[:, pl.ds(pl.multiple_of(base + 2 * width, 128), 128)] = dv.astype(BF)


def attn_fwd(qkv, seq, scale):
    tokens, width = qkv.shape[0], qkv.shape[1] // 3
    pairs = width // 128
    spec = lambda off: pl.BlockSpec((seq, 128), lambda b, j: (b, off + j))
    return pl.pallas_call(
        functools.partial(attn_fwd_kernel, scale),
        grid=(tokens // seq, pairs),
        in_specs=[spec(0), spec(pairs), spec(2 * pairs)],
        out_specs=spec(0),
        out_shape=jax.ShapeDtypeStruct((tokens, width), BF),
        cost_estimate=pl.CostEstimate(flops=int(2e10), bytes_accessed=4 * tokens * width * 2, transcendentals=0),
        name="attn_fwd",
    )(qkv, qkv, qkv)


def attn_bwd(qkv, do, seq, scale):
    tokens, width = qkv.shape[0], qkv.shape[1] // 3
    pairs = width // 128
    spec = lambda off: pl.BlockSpec((seq, 128), lambda b, j: (b, off + j))
    return pl.pallas_call(
        functools.partial(attn_bwd_kernel, scale, width),
        grid=(tokens // seq, pairs),
        in_specs=[spec(0), spec(pairs), spec(2 * pairs), spec(0)],
        out_specs=pl.BlockSpec((seq, 3 * width), lambda b, j: (b, 0)),
        out_shape=jax.ShapeDtypeStruct((tokens, 3 * width), BF),
        cost_estimate=pl.CostEstimate(flops=int(5e10), bytes_accessed=7 * tokens * width * 2, transcendentals=0),
        name="attn_bwd",
    )(qkv, qkv, qkv, do)


def layer_forward(hidden, weights, seq, scale):
    w_qkv, w_proj, w_up, w_down = weights
    hid_f32 = hidden.astype(F32)
    normed = rms_norm(hid_f32).astype(BF)
    qkv = dot(normed, w_qkv).astype(BF)
    attn = attn_fwd(qkv, seq, scale)
    mid = (hid_f32 + dot(attn, w_proj)).astype(BF)
    mid_f32 = mid.astype(F32)
    normed2 = rms_norm(mid_f32).astype(BF)
    up = dot(normed2, w_up).astype(BF)
    gelu = gelu_tanh(up.astype(F32)).astype(BF)
    out = (mid_f32 + dot(gelu, w_down)).astype(BF)
    return out, (hidden, normed, qkv, attn, mid, normed2, up, gelu)


def layer_backward(saved, ct_out, weights, seq, scale, need_input):
    w_qkv, w_proj, w_up, w_down = weights
    hidden, normed, qkv, attn, mid, normed2, up, gelu = saved
    g_down = dot_tn(gelu, ct_out)
    ct_gelu = dot_nt(ct_out, w_down).astype(BF)
    ct_up = jax.vjp(gelu_tanh, up.astype(F32))[1](ct_gelu.astype(F32))[0].astype(BF)
    g_up = dot_tn(normed2, ct_up)
    ct_norm2 = dot_nt(ct_up, w_up).astype(BF)
    ct_mid = (ct_out.astype(F32) + jax.vjp(rms_norm, mid.astype(F32))[1](ct_norm2.astype(F32))[0]).astype(BF)
    g_proj = dot_tn(attn, ct_mid)
    ct_attn = dot_nt(ct_mid, w_proj).astype(BF)
    ct_qkv = attn_bwd(qkv, ct_attn, seq, scale)
    g_qkv = dot_tn(normed, ct_qkv)
    ct_hidden = None
    if need_input:
        ct_norm = dot_nt(ct_qkv, w_qkv).astype(BF)
        ct_hidden = (ct_mid.astype(F32) + jax.vjp(rms_norm, hidden.astype(F32))[1](ct_norm.astype(F32))[0]).astype(BF)
    return ct_hidden, (g_qkv, g_proj, g_up, g_down)


def solution(mesh):
    stages = mesh.shape['pp']
    grid = Mesh(mesh.devices.reshape(2, 4, 4, 4), ("pp", "z", "y", "x"))
    dp = ("z", "y", "x")
    swap = [(0, 1), (1, 0)]

    def device_step(act_in, loss_seed, w_qkv, w_proj, w_up, w_down):
        micro, _, seq, d = act_in.shape
        mine = micro // 2
        pp = lax.axis_index('pp')
        heads3, hd = w_qkv.shape[2:]
        scale = hd ** -0.5

        def gather(w):
            flat = w.reshape(w.shape[1], -1)
            full = lax.all_gather(flat, ("pp",) + dp, axis=0, tiled=True)
            return full.reshape(2, full.shape[0] // 2, full.shape[1])

        full = [gather(w) for w in (w_qkv, w_proj, w_up, w_down)]
        layers = [[w[i] for w in full] for i in range(2)]
        act = lax.dynamic_slice_in_dim(act_in, pp * mine, mine, 0).reshape(mine * seq, d)
        seed = lax.dynamic_slice_in_dim(loss_seed, pp * mine, mine, 0).reshape(mine * seq, d)
        h1, saved0 = layer_forward(act, layers[0], seq, scale)
        h2, saved1 = layer_forward(h1, layers[1], seq, scale)

        out4 = h2.reshape(mine, 1, seq, d)
        half = seq // 2
        keep = lax.dynamic_slice_in_dim(out4, pp * half, half, 2)
        give = lax.dynamic_slice_in_dim(out4, (1 - pp) * half, half, 2)
        got = lax.ppermute(give, 'pp', swap)
        act_out = jnp.concatenate([jnp.where(pp == 0, keep, got), jnp.where(pp == 0, got, keep)], axis=0)

        ct1, grads1 = layer_backward(saved1, seed, layers[1], seq, scale, True)
        _, grads0 = layer_backward(saved0, ct1, layers[0], seq, scale, False)

        def reduce(g):
            rows, cols = g.shape
            h = cols // 2
            keep = lax.dynamic_slice_in_dim(g, pp * h, h, 1)
            give = lax.dynamic_slice_in_dim(g, (1 - pp) * h, h, 1)
            part = keep + lax.ppermute(give, 'pp', swap)
            for axis in dp:
                part = lax.psum_scatter(part, axis, scatter_dimension=0, tiled=True)
            return part

        def finish(p0, p1):
            keep = jnp.where(pp == 0, p0, p1)
            give = jnp.where(pp == 0, p1, p0)
            got = lax.ppermute(give, 'pp', swap)
            return jnp.concatenate([jnp.where(pp == 0, keep, got), jnp.where(pp == 0, got, keep)], axis=1)

        red1 = [reduce(g) for g in grads1]
        red0 = [reduce(g) for g in grads0]
        outs = [finish(a, b) for a, b in zip(red0, red1)]
        return tuple(o.reshape(w.shape) for o, w in zip(outs, (w_qkv, w_proj, w_up, w_down))) + (act_out,)

    weight_spec = P('pp', dp)
    act_spec = P(None, dp)
    return jax.shard_map(device_step, mesh=grid, in_specs=(act_spec, act_spec) + (weight_spec,) * 4, out_specs=(weight_spec,) * 4 + (P(None, dp, 'pp'),), check_vma=False)
```

```python
import functools

import jax
import jax.numpy as jnp
from jax import lax
from jax.experimental import pallas as pl
from jax.experimental.pallas import tpu as pltpu
from jax.sharding import Mesh
from jax.sharding import PartitionSpec as P

NORM_EPS = 1e-6
BF = jnp.bfloat16
F32 = jnp.float32


def rms_norm(hidden):
    return hidden * lax.rsqrt(jnp.mean(hidden * hidden, axis=-1, keepdims=True) + NORM_EPS)


def gelu_tanh(pre_act):
    return jax.nn.gelu(pre_act, approximate=True)


def dot(a, b):
    return lax.dot_general(a, b, (((1,), (0,)), ((), ())), preferred_element_type=F32)


def dot_nt(a, b):
    return lax.dot_general(a, b, (((1,), (1,)), ((), ())), preferred_element_type=F32)


def dot_tn(a, b):
    return lax.dot_general(a, b, (((0,), (0,)), ((), ())), preferred_element_type=F32)


def softmax_rows(q, kh, scale):
    s = dot_nt(q, kh) * scale
    row = lax.broadcasted_iota(jnp.int32, s.shape, 0)
    col = lax.broadcasted_iota(jnp.int32, s.shape, 1)
    s = jnp.where(row >= col, s, -1e30)
    e = jnp.exp(s - jnp.max(s, axis=-1, keepdims=True))
    return e * (1.0 / jnp.sum(e, axis=-1, keepdims=True))


def attn_fwd_kernel(scale, q_ref, k_ref, v_ref, o_ref):
    q, k, v = q_ref[...], k_ref[...], v_ref[...]
    low = lax.broadcasted_iota(jnp.int32, k.shape, 1) < 64
    zero = jnp.zeros_like(k)
    out = jnp.zeros(q.shape, F32)
    for half in range(2):
        keep = low if half == 0 else jnp.logical_not(low)
        p = softmax_rows(q, jnp.where(keep, k, zero), scale).astype(BF)
        out = out + dot(p, jnp.where(keep, v, zero))
    o_ref[...] = out.astype(BF)


def attn_bwd_kernel(scale, width, q_ref, k_ref, v_ref, do_ref, dqkv_ref):
    q, k, v, do = q_ref[...], k_ref[...], v_ref[...], do_ref[...]
    low = lax.broadcasted_iota(jnp.int32, k.shape, 1) < 64
    zero = jnp.zeros_like(k)
    dq = jnp.zeros(q.shape, F32)
    dk = jnp.zeros(q.shape, F32)
    dv = jnp.zeros(q.shape, F32)
    for half in range(2):
        keep = low if half == 0 else jnp.logical_not(low)
        kh, vh = jnp.where(keep, k, zero), jnp.where(keep, v, zero)
        qh, doh = jnp.where(keep, q, zero), jnp.where(keep, do, zero)
        p = softmax_rows(q, kh, scale)
        dp = dot_nt(do, vh).astype(BF).astype(F32)
        delta = jnp.sum(dp * p, axis=-1, keepdims=True)
        ds = (p * (dp - delta) * scale).astype(BF)
        dq = dq + dot(ds, kh)
        dk = dk + dot_tn(ds, qh)
        dv = dv + dot_tn(p.astype(BF), doh)
    base = pl.program_id(1) * 128
    dqkv_ref[:, pl.ds(pl.multiple_of(base, 128), 128)] = dq.astype(BF)
    dqkv_ref[:, pl.ds(pl.multiple_of(base + width, 128), 128)] = dk.astype(BF)
    dqkv_ref[:, pl.ds(pl.multiple_of(base + 2 * width, 128), 128)] = dv.astype(BF)


def attn_fwd(qkv, seq, scale):
    tokens, width = qkv.shape[0], qkv.shape[1] // 3
    pairs = width // 128
    spec = lambda off: pl.BlockSpec((seq, 128), lambda b, j: (b, off + j))
    return pl.pallas_call(
        functools.partial(attn_fwd_kernel, scale),
        grid=(tokens // seq, pairs),
        in_specs=[spec(0), spec(pairs), spec(2 * pairs)],
        out_specs=spec(0),
        out_shape=jax.ShapeDtypeStruct((tokens, width), BF),
        cost_estimate=pl.CostEstimate(flops=int(2e10), bytes_accessed=4 * tokens * width * 2, transcendentals=0),
        name="attn_fwd",
    )(qkv, qkv, qkv)


def attn_bwd(qkv, do, seq, scale):
    tokens, width = qkv.shape[0], qkv.shape[1] // 3
    pairs = width // 128
    spec = lambda off: pl.BlockSpec((seq, 128), lambda b, j: (b, off + j))
    return pl.pallas_call(
        functools.partial(attn_bwd_kernel, scale, width),
        grid=(tokens // seq, pairs),
        in_specs=[spec(0), spec(pairs), spec(2 * pairs), spec(0)],
        out_specs=pl.BlockSpec((seq, 3 * width), lambda b, j: (b, 0)),
        out_shape=jax.ShapeDtypeStruct((tokens, 3 * width), BF),
        cost_estimate=pl.CostEstimate(flops=int(5e10), bytes_accessed=7 * tokens * width * 2, transcendentals=0),
        name="attn_bwd",
    )(qkv, qkv, qkv, do)


def layer_forward(hidden, weights, seq, scale):
    w_qkv, w_proj, w_up, w_down = weights
    hid_f32 = hidden.astype(F32)
    normed = rms_norm(hid_f32).astype(BF)
    qkv = dot(normed, w_qkv).astype(BF)
    attn = attn_fwd(qkv, seq, scale)
    mid = (hid_f32 + dot(attn, w_proj)).astype(BF)
    mid_f32 = mid.astype(F32)
    normed2 = rms_norm(mid_f32).astype(BF)
    up = dot(normed2, w_up).astype(BF)
    gelu = gelu_tanh(up.astype(F32)).astype(BF)
    out = (mid_f32 + dot(gelu, w_down)).astype(BF)
    return out, (hidden, normed, qkv, attn, mid, normed2, up, gelu)


def layer_backward(saved, ct_out, weights, seq, scale, need_input):
    w_qkv, w_proj, w_up, w_down = weights
    hidden, normed, qkv, attn, mid, normed2, up, gelu = saved
    g_down = dot_tn(gelu, ct_out)
    ct_gelu = dot_nt(ct_out, w_down).astype(BF)
    ct_up = jax.vjp(gelu_tanh, up.astype(F32))[1](ct_gelu.astype(F32))[0].astype(BF)
    g_up = dot_tn(normed2, ct_up)
    ct_norm2 = dot_nt(ct_up, w_up).astype(BF)
    ct_mid = (ct_out.astype(F32) + jax.vjp(rms_norm, mid.astype(F32))[1](ct_norm2.astype(F32))[0]).astype(BF)
    g_proj = dot_tn(attn, ct_mid)
    ct_attn = dot_nt(ct_mid, w_proj).astype(BF)
    ct_qkv = attn_bwd(qkv, ct_attn, seq, scale)
    g_qkv = dot_tn(normed, ct_qkv)
    ct_hidden = None
    if need_input:
        ct_norm = dot_nt(ct_qkv, w_qkv).astype(BF)
        ct_hidden = (ct_mid.astype(F32) + jax.vjp(rms_norm, hidden.astype(F32))[1](ct_norm.astype(F32))[0]).astype(BF)
    return ct_hidden, (g_qkv, g_proj, g_up, g_down)


MESH = pl.DeviceIdType.MESH
AXES = ("z", "y", "x")
GATHER_ORDER = ((2, 1, 0), (0, 2, 1), (1, 0, 2))
REDUCE_ORDER = ((0, 1, 2), (1, 2, 0), (2, 0, 1))


def step_coord(pos, by):
    return lax.rem(pos + by, 4)


def neighbour(me, axis, by):
    return {AXES[axis]: step_coord(me[axis], by)}


def enter(me, partner):
    barrier = pltpu.get_barrier_semaphore()
    for axis in range(3):
        for by in (1, 3):
            pl.semaphore_signal(barrier, inc=1, device_id=neighbour(me, axis, by), device_id_type=MESH)
    pl.semaphore_signal(barrier, inc=1, device_id={"pp": partner}, device_id_type=MESH)
    pl.semaphore_wait(barrier, 7)


def remote(src, dst, send, recv, where):
    copy = pltpu.make_async_remote_copy(src_ref=src, dst_ref=dst, send_sem=send, recv_sem=recv, device_id=where, device_id_type=MESH)
    copy.start()
    return copy


def gather_kernel(up_ref, down_ref, qkv_ref, proj_ref, wup, wdown, wqkv, wproj, local_sem, send_sem, recv_sem, psend_sem, precv_sem):
    pp = lax.axis_index("pp")
    partner = 1 - pp
    me = tuple(lax.axis_index(a) for a in AXES)
    arrays = ((0, up_ref, wup), (1, down_ref, wdown), (2, qkv_ref, wqkv), (2, proj_ref, wproj))

    def half_of(ref, half):
        rows, cols = ref.shape[-2:]
        lead = (slice(None),) * (len(ref.shape) - 2)
        if rows > 8:
            return ref.at[lead + (pl.ds(half * (rows // 2), rows // 2), slice(None))]
        return ref.at[lead + (slice(None), pl.ds(half * (cols // 2), cols // 2))]

    def block(n, phase, where):
        group, _, out = arrays[n]
        order = GATHER_ORDER[group]
        idx = [None, None, None]
        for later, axis in enumerate(order):
            idx[axis] = slice(None) if later < phase else (where if later == phase else me[axis])
        return out.at[(pp,) + tuple(idx)]

    for n, (_, src, out) in enumerate(arrays):
        pltpu.make_async_copy(src, out.at[(pp,) + me], local_sem.at[n]).start()
    enter(me, partner)
    for n, (_, src, out) in enumerate(arrays):
        pltpu.make_async_copy(src, out.at[(pp,) + me], local_sem.at[n]).wait()

    sends = []
    partners = []

    def tell_partner(ref, n, slot):
        copy = remote(ref, ref, psend_sem.at[n, slot], precv_sem.at[n, slot], {"pp": partner})
        partners.append(copy)

    def send(ref, n, phase, slot, by):
        axis = GATHER_ORDER[arrays[n][0]][phase]
        copy = remote(ref, ref, send_sem.at[n, phase, slot], recv_sem.at[n, phase, slot], neighbour(me, axis, by))
        sends.append(copy)

    def arrived(ref, n, phase, slot):
        pltpu.make_async_copy(ref, ref, recv_sem.at[n, phase, slot]).wait()

    for phase in range(3):
        last = phase == 2
        place = [me[GATHER_ORDER[arrays[n][0]][phase]] for n in range(4)]
        for n in range(4):
            mine = block(n, phase, place[n])
            send(half_of(mine, 0), n, phase, 0, 1)
            send(half_of(mine, 1), n, phase, 1, 3)
        for n in range(4):
            mine = block(n, phase, place[n])
            send(half_of(mine, 1), n, phase, 2, 1)
            send(half_of(mine, 0), n, phase, 3, 3)
            if last:
                tell_partner(mine, n, 0)
        for n in range(4):
            left = block(n, phase, step_coord(place[n], 3))
            right = block(n, phase, step_coord(place[n], 1))
            arrived(half_of(left, 0), n, phase, 0)
            send(half_of(left, 0), n, phase, 4, 1)
            if last:
                tell_partner(half_of(left, 0), n, 1)
            arrived(half_of(right, 1), n, phase, 1)
            send(half_of(right, 1), n, phase, 5, 3)
            if last:
                tell_partner(half_of(right, 1), n, 2)
        for n in range(4):
            left = block(n, phase, step_coord(place[n], 3))
            right = block(n, phase, step_coord(place[n], 1))
            arrived(half_of(left, 1), n, phase, 2)
            if last:
                tell_partner(half_of(left, 1), n, 3)
            arrived(half_of(right, 0), n, phase, 3)
            if last:
                tell_partner(half_of(right, 0), n, 4)
        for n in range(4):
            far = block(n, phase, step_coord(place[n], 2))
            arrived(half_of(far, 0), n, phase, 4)
            if last:
                tell_partner(half_of(far, 0), n, 5)
            arrived(half_of(far, 1), n, phase, 5)
            if last:
                tell_partner(half_of(far, 1), n, 6)
    for copy in sends:
        copy.wait_send()
    for copy in partners:
        copy.wait_send()
    for copy in partners:
        copy.wait_recv()


def gather_weights(w_qkv, w_proj, w_up, w_down):
    vmem = pl.BlockSpec(memory_space=pltpu.VMEM)
    full = lambda w: jax.ShapeDtypeStruct((2, 4, 4, 4) + w.shape, BF)
    dma = pltpu.SemaphoreType.DMA
    args = (w_up, w_down, w_qkv, w_proj)
    outs = pl.pallas_call(
        gather_kernel,
        in_specs=[vmem] * 4,
        out_specs=[vmem] * 4,
        out_shape=[full(w) for w in args],
        scratch_shapes=[dma((4,)), dma((4, 3, 6)), dma((4, 3, 6)), dma((4, 7)), dma((4, 7))],
        compiler_params=pltpu.CompilerParams(collective_id=0, has_side_effects=True, vmem_limit_bytes=40 << 20),
        name="gather_weights",
    )(*args)
    flat = [o.reshape(2, -1, o.shape[-1]) for o in outs]
    return flat[2], flat[3], flat[0], flat[1]


def reduce_kernel(up_ref, down_ref, qkv_ref, proj_ref, oup, odown, oqkv, oproj,
                  acc, peer, t1a, t2a, t1b, t2b, t1c, t2c,
                  load_sem, psend_sem, precv_sem, send_sem, recv_sem, fsend_sem, frecv_sem):
    pp = lax.axis_index("pp")
    partner = 1 - pp
    me = tuple(lax.axis_index(a) for a in AXES)
    t1s, t2s = (t1a, t1b, t1c), (t2a, t2b, t2c)

    def pieces(color, core):
        if color == 0:
            return [(up_ref, pl.ds(0, 8), pl.ds(pl.multiple_of(core * 1024 + h * 512, 128), 512), h, pl.ds(0, 512)) for h in range(2)]
        if color == 1:
            return [(down_ref, pl.ds(pl.multiple_of(core * 16 + h * 8, 8), 8), pl.ds(0, 512), h, pl.ds(0, 512)) for h in range(2)]
        return [
            (qkv_ref, pl.ds(0, 8), pl.ds(pl.multiple_of(core * 768, 128), 512), 0, pl.ds(0, 512)),
            (qkv_ref, pl.ds(0, 8), pl.ds(pl.multiple_of(core * 768 + 512, 128), 256), 1, pl.ds(0, 256)),
            (proj_ref, pl.ds(0, 8), pl.ds(pl.multiple_of(core * 256, 128), 256), 1, pl.ds(256, 256)),
        ]

    def lead(color, phase, where):
        order = REDUCE_ORDER[color]
        idx = [None, None, None]
        for later, axis in enumerate(order):
            idx[axis] = me[axis] if later < phase else (where if later == phase else slice(None))
        return tuple(idx)

    def place(color, phase, by):
        return step_coord(me[REDUCE_ORDER[color][phase]], by)

    def loads(color, pos, by):
        where = lead(color, 0, place(color, 0, by))
        return [
            pltpu.make_async_copy(ref.at[where + (rows, cols)], acc.at[(color,) + where + (h, slice(None), into)], load_sem.at[color, pos, n])
            for n, (ref, rows, cols, h, into) in enumerate(pieces(color, pp))
        ]

    def swaps(color, pos, by):
        where = lead(color, 0, place(color, 0, by))
        return [
            pltpu.make_async_remote_copy(
                src_ref=ref.at[where + (rows, cols)], dst_ref=peer.at[(color,) + where + (h, slice(None), into)],
                send_sem=psend_sem.at[color, pos, n], recv_sem=precv_sem.at[color, pos, n], device_id={"pp": partner}, device_id_type=MESH)
            for n, (ref, rows, cols, h, into) in enumerate(pieces(color, partner))
        ]

    def add_block(dst, src):
        dims = dst.shape[:-2]
        total = 1
        for s in dims:
            total *= s

        def one(index):
            dst[index] = dst[index] + src[index]

        if total <= 4:
            for flat in range(total):
                index, rest = [], flat
                for s in reversed(dims):
                    index.append(rest % s)
                    rest //= s
                one(tuple(reversed(index)))
            return

        def body(i, _):
            inner = dims[1:]
            count = total // dims[0]
            for flat in range(count):
                index, rest = [], flat
                for s in reversed(inner):
                    index.append(rest % s)
                    rest //= s
                one((i,) + tuple(reversed(index)))
            return 0

        lax.fori_loop(0, dims[0], body, 0)

    offsets = (2, 1, 3, 0)
    for pos, by in enumerate(offsets):
        for color in range(3):
            for copy in loads(color, pos, by):
                copy.start()
    enter(me, partner)
    for pos, by in enumerate(offsets):
        for color in range(3):
            for copy in swaps(color, pos, by):
                copy.start()

    sends = []

    def send(color, phase, slot, src, dst, by):
        axis = REDUCE_ORDER[color][phase]
        sends.append(remote(src, dst, send_sem.at[color, phase, slot], recv_sem.at[color, phase, slot], neighbour(me, axis, by)))

    def arrived(color, phase, slot, ref):
        pltpu.make_async_copy(ref, ref, recv_sem.at[color, phase, slot]).wait()

    def part(color, phase, by, half):
        return acc.at[(color,) + lead(color, phase, place(color, phase, by)) + (half,)]

    def slot1(color, phase, side):
        return t1s[phase].at[color, side]

    def slot2(color, phase, side, half):
        return t2s[phase].at[color, side, half]

    def first_sends(color, phase, by):
        if by == 2:
            send(color, phase, 0, part(color, phase, 2, 0), slot1(color, phase, 0), 1)
            send(color, phase, 1, part(color, phase, 2, 1), slot1(color, phase, 1), 3)
        if by == 1:
            send(color, phase, 2, part(color, phase, 1, 1), slot2(color, phase, 0, 1), 1)
        if by == 3:
            send(color, phase, 3, part(color, phase, 3, 0), slot2(color, phase, 1, 0), 3)

    for pos, by in enumerate(offsets):
        for color in range(3):
            for copy in loads(color, pos, by):
                copy.wait()
            for copy in swaps(color, pos, by):
                copy.wait_recv()
            where = lead(color, 0, place(color, 0, by))
            add_block(acc.at[(color,) + where], peer.at[(color,) + where])
            first_sends(color, 0, by)

    for phase in range(3):
        if phase:
            for by in (2, 1, 3):
                for color in range(3):
                    first_sends(color, phase, by)
        for color in range(3):
            arrived(color, phase, 0, slot1(color, phase, 0))
            add_block(part(color, phase, 1, 0), slot1(color, phase, 0))
            send(color, phase, 4, part(color, phase, 1, 0), slot2(color, phase, 0, 0), 1)
            arrived(color, phase, 1, slot1(color, phase, 1))
            add_block(part(color, phase, 3, 1), slot1(color, phase, 1))
            send(color, phase, 5, part(color, phase, 3, 1), slot2(color, phase, 1, 1), 3)
        for color in range(3):
            arrived(color, phase, 2, slot2(color, phase, 0, 1))
            add_block(part(color, phase, 0, 1), slot2(color, phase, 0, 1))
            arrived(color, phase, 3, slot2(color, phase, 1, 0))
            add_block(part(color, phase, 0, 0), slot2(color, phase, 1, 0))
        for color in range(3):
            arrived(color, phase, 4, slot2(color, phase, 0, 0))
            add_block(part(color, phase, 0, 0), slot2(color, phase, 0, 0))
            arrived(color, phase, 5, slot2(color, phase, 1, 1))
            add_block(part(color, phase, 0, 1), slot2(color, phase, 1, 1))

    outs = {id(up_ref): oup, id(down_ref): odown, id(qkv_ref): oqkv, id(proj_ref): oproj}
    finals = []
    for color in range(3):
        for n, (ref, rows, cols, h, into) in enumerate(pieces(color, pp)):
            out = outs[id(ref)]
            src = acc.at[(color,) + me + (h, slice(None), into)]
            dst = out.at[rows, cols]
            dst[...] = src[...]
            finals.append(remote(src, dst, fsend_sem.at[color, n], frecv_sem.at[color, n], {"pp": partner}))
    for copy in finals:
        copy.wait_send()
        copy.wait_recv()
    for copy in sends:
        copy.wait_send()
    for pos, by in enumerate(offsets):
        for color in range(3):
            for copy in swaps(color, pos, by):
                copy.wait_send()


def reduce_grads(grads, which):
    g_qkv, g_proj, g_up, g_down = grads
    args = [g.reshape(4, 4, 4, g.shape[0] // 64, g.shape[1]) for g in (g_up, g_down, g_qkv, g_proj)]
    vmem, dma = pltpu.VMEM, pltpu.SemaphoreType.DMA
    outs = pl.pallas_call(
        reduce_kernel,
        in_specs=[pl.BlockSpec(memory_space=pl.ANY)] * 4,
        out_specs=[pl.BlockSpec(memory_space=vmem)] * 4,
        out_shape=[jax.ShapeDtypeStruct(a.shape[3:], F32) for a in args],
        scratch_shapes=[
            vmem((3, 4, 4, 4, 2, 8, 512), F32), vmem((3, 4, 4, 4, 2, 8, 512), F32),
            vmem((3, 2, 4, 4, 8, 512), F32), vmem((3, 2, 2, 4, 4, 8, 512), F32),
            vmem((3, 2, 4, 8, 512), F32), vmem((3, 2, 2, 4, 8, 512), F32),
            vmem((3, 2, 8, 512), F32), vmem((3, 2, 2, 8, 512), F32),
            dma((3, 4, 3)), dma((3, 4, 3)), dma((3, 4, 3)), dma((3, 3, 6)), dma((3, 3, 6)), dma((3, 3)), dma((3, 3)),
        ],
        compiler_params=pltpu.CompilerParams(collective_id=1 + which, has_side_effects=True, vmem_limit_bytes=30 << 20),
        name=f"reduce_grads_{which}",
    )(*args)
    return outs[2], outs[3], outs[0], outs[1]


def solution(mesh):
    stages = mesh.shape['pp']
    grid = Mesh(mesh.devices.reshape(2, 4, 4, 4), ("pp", "z", "y", "x"))
    dp = ("z", "y", "x")
    swap = [(0, 1), (1, 0)]

    def device_step(act_in, loss_seed, w_qkv, w_proj, w_up, w_down):
        micro, _, seq, d = act_in.shape
        mine = micro // 2
        pp = lax.axis_index('pp')
        heads3, hd = w_qkv.shape[2:]
        scale = hd ** -0.5

        full = gather_weights(*(w.reshape(w.shape[1], -1) for w in (w_qkv, w_proj, w_up, w_down)))
        layers = [[w[i] for w in full] for i in range(2)]
        act = lax.dynamic_slice_in_dim(act_in, pp * mine, mine, 0).reshape(mine * seq, d)
        seed = lax.dynamic_slice_in_dim(loss_seed, pp * mine, mine, 0).reshape(mine * seq, d)
        h1, saved0 = layer_forward(act, layers[0], seq, scale)
        h2, saved1 = layer_forward(h1, layers[1], seq, scale)

        out4 = h2.reshape(mine, 1, seq, d)
        half = seq // 2
        keep = lax.dynamic_slice_in_dim(out4, pp * half, half, 2)
        give = lax.dynamic_slice_in_dim(out4, (1 - pp) * half, half, 2)
        got = lax.ppermute(give, 'pp', swap)
        act_out = jnp.concatenate([jnp.where(pp == 0, keep, got), jnp.where(pp == 0, got, keep)], axis=0)

        ct1, grads1 = layer_backward(saved1, seed, layers[1], seq, scale, True)
        _, grads0 = layer_backward(saved0, ct1, layers[0], seq, scale, False)

        red1 = reduce_grads(grads1, 1)
        red0 = reduce_grads(grads0, 0)
        outs = [jnp.where(pp == 0, a, b) for a, b in zip(red0, red1)]
        return tuple(o.reshape(w.shape) for o, w in zip(outs, (w_qkv, w_proj, w_up, w_down))) + (act_out,)

    weight_spec = P('pp', dp)
    act_spec = P(None, dp)
    return jax.shard_map(device_step, mesh=grid, in_specs=(act_spec, act_spec) + (weight_spec,) * 4, out_specs=(weight_spec,) * 4 + (P(None, dp, 'pp'),), check_vma=False)
```

```python
import functools

import jax
import jax.numpy as jnp
from jax import lax
from jax.experimental import pallas as pl
from jax.experimental.pallas import tpu as pltpu
from jax.sharding import Mesh
from jax.sharding import PartitionSpec as P

NORM_EPS = 1e-6
BF = jnp.bfloat16
F32 = jnp.float32


def rms_norm(hidden):
    return hidden * lax.rsqrt(jnp.mean(hidden * hidden, axis=-1, keepdims=True) + NORM_EPS)


def dot(a, b):
    return lax.dot_general(a, b, (((1,), (0,)), ((), ())), preferred_element_type=F32)


def dot_nt(a, b):
    return lax.dot_general(a, b, (((1,), (1,)), ((), ())), preferred_element_type=F32)


def dot_tn(a, b):
    return lax.dot_general(a, b, (((0,), (0,)), ((), ())), preferred_element_type=F32)


LOG2E = 1.4426950408889634
GELU_A = 0.7978845608028654
GELU_B = GELU_A * 0.044715


def split_heads(refs, count):
    low = lax.broadcasted_iota(jnp.int32, (refs[0].shape[0], 128), 1) < 64
    zero = jnp.zeros((refs[0].shape[0], 128), BF)
    heads = []
    for h in range(count):
        keep = low if h % 2 == 0 else jnp.logical_not(low)
        lanes = slice((h // 2) * 128, (h // 2) * 128 + 128)
        heads.append([(r[:, lanes], jnp.where(keep, r[:, lanes], zero)) for r in refs])
    return heads


def causal_mask(n):
    return lax.broadcasted_iota(jnp.int32, (n, n), 0) >= lax.broadcasted_iota(jnp.int32, (n, n), 1)


def softmax_rows(s, keep, scale):
    s = jnp.where(keep, s, -1e30)
    e = jnp.exp2((s - jnp.max(s, axis=-1, keepdims=True)) * (scale * LOG2E))
    return e * (1.0 / jnp.sum(e, axis=-1, keepdims=True))


def row_blocks(seq, parts):
    return parts if seq == parts[-1][1] else ((0, seq),)


def attn_fwd_kernel(scale, q_ref, k_ref, v_ref, o_ref):
    seq, lanes = q_ref.shape
    count = lanes // 64
    blocks = row_blocks(seq, ((0, 128), (128, 256), (256, 384)))
    keep = causal_mask(seq)
    heads = split_heads((q_ref, k_ref, v_ref), count)
    scores = [[dot_nt(q[0][a:b], k[1][:b]) for a, b in blocks] for q, k, v in heads]
    probs = [[softmax_rows(s, keep[a:b, :b], scale).astype(BF) for (a, b), s in zip(blocks, row)] for row in scores]
    for h in range(0, count, 2):
        for n, (a, b) in enumerate(blocks):
            pair = dot(probs[h][n], heads[h][2][1][:b]) + dot(probs[h + 1][n], heads[h + 1][2][1][:b])
            o_ref[a:b, (h // 2) * 128:(h // 2) * 128 + 128] = pair.astype(BF)


def attn_bwd_kernel(scale, width, q_ref, k_ref, v_ref, do_ref, dqkv_ref):
    seq, lanes = q_ref.shape
    count = lanes // 64
    blocks = row_blocks(seq, ((0, 256), (256, 384)))
    keep = causal_mask(seq)
    base = pl.program_id(1) * lanes
    heads = split_heads((q_ref, k_ref, v_ref, do_ref), count)
    firsts = [[(dot_nt(q[0][a:b], k[1][:b]), dot_nt(do[0][a:b], v[1][:b])) for a, b in blocks] for q, k, v, do in heads]
    work = []
    for row in firsts:
        done = []
        for (a, b), (s, dp) in zip(blocks, row):
            p = softmax_rows(s, keep[a:b, :b], scale)
            dp = dp.astype(BF).astype(F32)
            delta = jnp.sum(dp * p, axis=-1, keepdims=True)
            done.append((p.astype(BF), (p * (dp - delta) * scale).astype(BF)))
        work.append(done)
    total = lambda terms: functools.reduce(lambda x, y: x + y, terms)
    for j in range(count // 2):
        pair = (2 * j, 2 * j + 1)
        cols = [pl.ds(pl.multiple_of(base + j * 128 + i * width, 128), 128) for i in range(3)]
        for n, (a, b) in enumerate(blocks):
            dqkv_ref[a:b, cols[0]] = total([dot(work[h][n][1], heads[h][1][1][:b]) for h in pair]).astype(BF)
        for i, (_, hi) in enumerate(blocks):
            lo = blocks[i - 1][1] if i else 0
            later = [(n, a, b, h) for n, (a, b) in enumerate(blocks) if n >= i for h in pair]
            dqkv_ref[lo:hi, cols[1]] = total([dot_tn(work[h][n][1][:, lo:hi], heads[h][0][1][a:b]) for n, a, b, h in later]).astype(BF)
            dqkv_ref[lo:hi, cols[2]] = total([dot_tn(work[h][n][0][:, lo:hi], heads[h][3][1][a:b]) for n, a, b, h in later]).astype(BF)


def attn_fwd(qkv, seq, scale):
    tokens, width = qkv.shape[0], qkv.shape[1] // 3
    spec = lambda off: pl.BlockSpec((seq, width), lambda b: (b, off))
    return pl.pallas_call(
        functools.partial(attn_fwd_kernel, scale),
        grid=(tokens // seq,),
        in_specs=[spec(0), spec(1), spec(2)],
        out_specs=spec(0),
        out_shape=jax.ShapeDtypeStruct((tokens, width), BF),
        name="attn_fwd",
    )(qkv, qkv, qkv)


def pre_kernel(h_ref, w_ref, n_ref, qkv_ref):
    normed = rms_norm(h_ref[...].astype(F32)).astype(BF)
    n_ref[...] = normed
    qkv_ref[...] = dot(normed, w_ref[...]).astype(BF)


def whole(shape, layer=None):
    block = shape if layer is None else (None,) + shape
    index = (0,) * len(shape) if layer is None else (layer,) + (0,) * len(shape)
    return pl.BlockSpec(block, lambda *_: index, pipeline_mode=pl.Buffered(1))


def pre_attn(hidden, w_qkv, layer, tile):
    tokens, d = hidden.shape
    cols = w_qkv.shape[2]
    row = lambda n: pl.BlockSpec((tile, n), lambda i: (i, 0))
    return pl.pallas_call(
        pre_kernel,
        grid=(tokens // tile,),
        in_specs=[row(d), whole((d, cols), layer)],
        out_specs=[row(d), row(cols)],
        out_shape=[jax.ShapeDtypeStruct((tokens, d), BF), jax.ShapeDtypeStruct((tokens, cols), BF)],
        name="pre_attn",
    )(hidden, w_qkv)


def post_kernel(h_ref, a_ref, wp_ref, wu_ref, wd_ref, mid_ref, n2_ref, up_ref, ge_ref, out_ref):
    mid = (h_ref[...].astype(F32) + dot(a_ref[...], wp_ref[...])).astype(BF)
    mid_ref[...] = mid
    mid_f32 = mid.astype(F32)
    n2 = rms_norm(mid_f32).astype(BF)
    n2_ref[...] = n2
    ff = wu_ref.shape[1]
    for c in range(0, ff, 512):
        up = dot(n2, wu_ref[:, c:c + 512]).astype(BF)
        up_ref[:, c:c + 512] = up
        u = up.astype(F32)
        t = jnp.tanh(u * (GELU_A + GELU_B * (u * u)))
        ge_ref[:, c:c + 512] = (u * (0.5 * t + 0.5)).astype(BF)
    out_ref[...] = (mid_f32 + dot(ge_ref[...], wd_ref[...])).astype(BF)


def post_attn(hidden, attn, w_proj, w_up, w_down, layer, tile):
    tokens, d = hidden.shape
    ff = w_up.shape[2]
    row = lambda n: pl.BlockSpec((tile, n), lambda i: (i, 0))
    sizes = (d, d, ff, ff, d)
    return pl.pallas_call(
        post_kernel,
        grid=(tokens // tile,),
        in_specs=[row(d), row(d), whole((d, d), layer), whole((d, ff), layer), whole((ff, d), layer)],
        out_specs=[row(n) for n in sizes],
        out_shape=[jax.ShapeDtypeStruct((tokens, n), BF) for n in sizes],
        name="post_attn",
    )(hidden, attn, w_proj, w_up, w_down)


def gelu_pull(u, g):
    u2 = u * u
    s = 0.5 * jnp.tanh(u * (GELU_A + GELU_B * u2)) + 0.5
    return g * (s + (s - s * s) * (u * (2 * GELU_A + (6 * GELU_B) * u2)))


def rms_pull(m, g):
    r = lax.rsqrt(jnp.mean(m * m, axis=-1, keepdims=True) + NORM_EPS)
    return g * r - m * (r * r * r * jnp.mean(g * m, axis=-1, keepdims=True))


MESH = pl.DeviceIdType.MESH
AXES = ("z", "y", "x")
GATHER_ORDER = ((2, 1, 0), (0, 2, 1), (1, 0, 2))
REDUCE_ORDER = ((0, 1, 2), (1, 2, 0), (2, 0, 1))


def step_coord(pos, by):
    return lax.rem(pos + by, 4)


def neighbour(me, axis, by):
    return {AXES[axis]: step_coord(me[axis], by)}


def enter(me, partner):
    barrier = pltpu.get_barrier_semaphore()
    for axis in range(3):
        for by in (1, 3):
            pl.semaphore_signal(barrier, inc=1, device_id=neighbour(me, axis, by), device_id_type=MESH)
    pl.semaphore_signal(barrier, inc=1, device_id={"pp": partner}, device_id_type=MESH)
    pl.semaphore_wait(barrier, 7)


def remote(src, dst, send, recv, where):
    copy = pltpu.make_async_remote_copy(src_ref=src, dst_ref=dst, send_sem=send, recv_sem=recv, device_id=where, device_id_type=MESH)
    copy.start()
    return copy


def gather_kernel(up_ref, down_ref, qkv_ref, proj_ref, wup, wdown, wqkv, wproj, local_sem, send_sem, recv_sem, psend_sem, precv_sem):
    pp = lax.axis_index("pp")
    partner = 1 - pp
    me = tuple(lax.axis_index(a) for a in AXES)
    arrays = ((0, up_ref, wup), (1, down_ref, wdown), (2, qkv_ref, wqkv), (2, proj_ref, wproj))

    def half_of(ref, half):
        rows, cols = ref.shape[-2:]
        lead = (slice(None),) * (len(ref.shape) - 2)
        if rows > 8:
            return ref.at[lead + (pl.ds(half * (rows // 2), rows // 2), slice(None))]
        return ref.at[lead + (slice(None), pl.ds(half * (cols // 2), cols // 2))]

    def block(n, phase, where):
        group, _, out = arrays[n]
        order = GATHER_ORDER[group]
        idx = [None, None, None]
        for later, axis in enumerate(order):
            idx[axis] = slice(None) if later < phase else (where if later == phase else me[axis])
        return out.at[(pp,) + tuple(idx)]

    for n, (_, src, out) in enumerate(arrays):
        pltpu.make_async_copy(src, out.at[(pp,) + me], local_sem.at[n]).start()
    enter(me, partner)
    for n, (_, src, out) in enumerate(arrays):
        pltpu.make_async_copy(src, out.at[(pp,) + me], local_sem.at[n]).wait()

    sends = []
    partners = []

    def tell_partner(ref, n, slot):
        copy = remote(ref, ref, psend_sem.at[n, slot], precv_sem.at[n, slot], {"pp": partner})
        partners.append(copy)

    def send(ref, n, phase, slot, by):
        axis = GATHER_ORDER[arrays[n][0]][phase]
        copy = remote(ref, ref, send_sem.at[n, phase, slot], recv_sem.at[n, phase, slot], neighbour(me, axis, by))
        sends.append(copy)

    def arrived(ref, n, phase, slot):
        pltpu.make_async_copy(ref, ref, recv_sem.at[n, phase, slot]).wait()

    for phase in range(3):
        last = phase == 2
        place = [me[GATHER_ORDER[arrays[n][0]][phase]] for n in range(4)]
        for n in range(4):
            mine = block(n, phase, place[n])
            send(half_of(mine, 0), n, phase, 0, 1)
            send(half_of(mine, 1), n, phase, 1, 3)
        for n in range(4):
            mine = block(n, phase, place[n])
            send(half_of(mine, 1), n, phase, 2, 1)
            send(half_of(mine, 0), n, phase, 3, 3)
            if last:
                tell_partner(mine, n, 0)
        for n in range(4):
            left = block(n, phase, step_coord(place[n], 3))
            right = block(n, phase, step_coord(place[n], 1))
            arrived(half_of(left, 0), n, phase, 0)
            send(half_of(left, 0), n, phase, 4, 1)
            if last:
                tell_partner(half_of(left, 0), n, 1)
            arrived(half_of(right, 1), n, phase, 1)
            send(half_of(right, 1), n, phase, 5, 3)
            if last:
                tell_partner(half_of(right, 1), n, 2)
        for n in range(4):
            left = block(n, phase, step_coord(place[n], 3))
            right = block(n, phase, step_coord(place[n], 1))
            arrived(half_of(left, 1), n, phase, 2)
            if last:
                tell_partner(half_of(left, 1), n, 3)
            arrived(half_of(right, 0), n, phase, 3)
            if last:
                tell_partner(half_of(right, 0), n, 4)
        for n in range(4):
            far = block(n, phase, step_coord(place[n], 2))
            arrived(half_of(far, 0), n, phase, 4)
            if last:
                tell_partner(half_of(far, 0), n, 5)
            arrived(half_of(far, 1), n, phase, 5)
            if last:
                tell_partner(half_of(far, 1), n, 6)
    for copy in sends:
        copy.wait_send()
    for copy in partners:
        copy.wait_send()
    for copy in partners:
        copy.wait_recv()


def gather_weights(w_qkv, w_proj, w_up, w_down):
    vmem = pl.BlockSpec(memory_space=pltpu.VMEM)
    full = lambda w: jax.ShapeDtypeStruct((2, 4, 4, 4) + w.shape, BF)
    dma = pltpu.SemaphoreType.DMA
    args = (w_up, w_down, w_qkv, w_proj)
    outs = pl.pallas_call(
        gather_kernel,
        in_specs=[vmem] * 4,
        out_specs=[vmem] * 4,
        out_shape=[full(w) for w in args],
        scratch_shapes=[dma((4,)), dma((4, 3, 6)), dma((4, 3, 6)), dma((4, 7)), dma((4, 7))],
        compiler_params=pltpu.CompilerParams(collective_id=0, has_side_effects=True, vmem_limit_bytes=40 << 20),
        name="gather_weights",
    )(*args)
    flat = [o.reshape(2, -1, o.shape[-1]) for o in outs]
    return flat[2], flat[3], flat[0], flat[1]


REDUCE_OFFSETS = (2, 1, 3, 0)


def reduce_pieces(refs, color, core):
    up_ref, down_ref, qkv_ref, proj_ref = refs
    if color == 0:
        return [(up_ref, pl.ds(0, 8), pl.ds(pl.multiple_of(core * 1024 + h * 512, 128), 512), h, pl.ds(0, 512)) for h in range(2)]
    if color == 1:
        return [(down_ref, pl.ds(pl.multiple_of(core * 16 + h * 8, 8), 8), pl.ds(0, 512), h, pl.ds(0, 512)) for h in range(2)]
    return [
        (qkv_ref, pl.ds(0, 8), pl.ds(pl.multiple_of(core * 768, 128), 512), 0, pl.ds(0, 512)),
        (qkv_ref, pl.ds(0, 8), pl.ds(pl.multiple_of(core * 768 + 512, 128), 256), 1, pl.ds(0, 256)),
        (proj_ref, pl.ds(0, 8), pl.ds(pl.multiple_of(core * 256, 128), 256), 1, pl.ds(256, 256)),
    ]


def add_block(out, dst, src):
    dims = dst.shape[:-2]
    total = 1
    for s in dims:
        total *= s

    def spread(flat, inner):
        index = []
        for s in reversed(inner):
            index.append(flat % s)
            flat //= s
        return tuple(reversed(index))

    def one(index):
        out[index] = dst[index] + src[index]

    if total <= 4:
        for flat in range(total):
            one(spread(flat, dims))
        return

    def body(i, _):
        for flat in range(total // dims[0]):
            one((i,) + spread(flat, dims[1:]))
        return 0

    lax.fori_loop(0, dims[0], body, 0)


class Reducer:
    def __init__(self, acc, slots, sems, start=0):
        self.pp = lax.axis_index("pp")
        self.partner = 1 - self.pp
        self.me = tuple(lax.axis_index(a) for a in AXES)
        self.acc, self.slots, self.start = acc, slots, start
        self.send_sem, self.recv_sem = sems

    def lead(self, color, phase, where):
        order = REDUCE_ORDER[color]
        idx = [None, None, None]
        for later, axis in enumerate(order):
            idx[axis] = self.me[axis] if later < phase else (where if later == phase else slice(None))
        return tuple(v for axis, v in enumerate(idx) if order.index(axis) >= self.start)

    def place(self, color, phase, by):
        return step_coord(self.me[REDUCE_ORDER[color][phase]], by)

    def loads(self, refs, sem, color, pos):
        where = self.lead(color, 0, self.place(color, 0, REDUCE_OFFSETS[pos]))
        return [
            pltpu.make_async_copy(ref.at[where + (rows, cols)], self.acc.at[(color,) + where + (h, slice(None), into)], sem.at[color, pos, n])
            for n, (ref, rows, cols, h, into) in enumerate(reduce_pieces(refs, color, self.pp))
        ]

    def swaps(self, refs, peer, sems, color, pos):
        where = self.lead(color, 0, self.place(color, 0, REDUCE_OFFSETS[pos]))
        return [
            pltpu.make_async_remote_copy(
                src_ref=ref.at[where + (rows, cols)], dst_ref=peer.at[(color,) + where + (h, slice(None), into)],
                send_sem=sems[0].at[color, pos, n], recv_sem=sems[1].at[color, pos, n], device_id={"pp": self.partner}, device_id_type=MESH)
            for n, (ref, rows, cols, h, into) in enumerate(reduce_pieces(refs, color, self.partner))
        ]

    def part(self, color, phase, by, half):
        return self.acc.at[(color,) + self.lead(color, phase, self.place(color, phase, by)) + (half,)]

    def near(self, color, phase, side):
        return self.slots[phase][0].at[color, side]

    def final(self, color, phase, side, half):
        return self.slots[phase][1].at[color, side, half]

    def copy(self, color, phase, n):
        part, near, final = self.part, self.near, self.final
        plan = (
            (part(color, phase, 2, 0), near(color, phase, 0), 1),
            (part(color, phase, 2, 1), near(color, phase, 1), 3),
            (part(color, phase, 1, 1), final(color, phase, 0, 1), 1),
            (part(color, phase, 3, 0), final(color, phase, 1, 0), 3),
            (part(color, phase, 1, 0), final(color, phase, 0, 0), 1),
            (part(color, phase, 3, 1), final(color, phase, 1, 1), 3),
        )
        k = phase - self.start
        src, dst, by = plan[n]
        return pltpu.make_async_remote_copy(
            src_ref=src, dst_ref=dst, send_sem=self.send_sem.at[color, k, n], recv_sem=self.recv_sem.at[color, k, n],
            device_id=neighbour(self.me, REDUCE_ORDER[color][phase], by), device_id_type=MESH)

    def first_sends(self, color, phase, by):
        for n in {2: (0, 1), 1: (2,), 3: (3,), 0: ()}[by]:
            self.copy(color, phase, n).start()

    def swapped(self, refs, peer, load_sem, swap_sems, pos):
        by = REDUCE_OFFSETS[pos]
        for color in range(3):
            for copy in self.loads(refs, load_sem, color, pos):
                copy.wait()
            for copy in self.swaps(refs, peer, swap_sems, color, pos):
                copy.wait_recv()
            block = self.acc.at[(color,) + self.lead(color, 0, self.place(color, 0, by))]
            add_block(block, block, peer.at[(color,) + self.lead(color, 0, self.place(color, 0, by))])
            self.first_sends(color, 0, by)

    def all_first(self, phase):
        for by in (2, 1, 3):
            for color in range(3):
                self.first_sends(color, phase, by)

    def second(self, phase):
        for color in range(3):
            for n, by, half in ((0, 1, 0), (1, 3, 1)):
                self.copy(color, phase, n).wait_recv()
                dst = self.part(color, phase, by, half)
                add_block(dst, dst, self.near(color, phase, n))
                self.copy(color, phase, n + 4).start()

    def third(self, phase):
        for color in range(3):
            for n, side, half in ((2, 0, 1), (3, 1, 0)):
                self.copy(color, phase, n).wait_recv()
                dst = self.part(color, phase, 0, half)
                add_block(dst, dst, self.final(color, phase, side, half))

    def fourth(self, phase, out=None):
        for color in range(3):
            for n, side, half in ((4, 0, 0), (5, 1, 1)):
                self.copy(color, phase, n).wait_recv()
                dst = self.part(color, phase, 0, half)
                add_block(dst if out is None else out.at[color, :, :, half], dst, self.final(color, phase, side, half))

    def drain(self, phase):
        for color in range(3):
            for n in range(6):
                self.copy(color, phase, n).wait_send()

    def finals(self, outs, sems):
        copies = []
        for color in range(3):
            for n, (out, rows, cols, h, into) in enumerate(reduce_pieces(outs, color, self.pp)):
                where = self.lead(color, 3, None)
                copies.append((out.at[rows, cols], self.acc.at[(color,) + where + (h, slice(None), into)], pltpu.make_async_remote_copy(
                    src_ref=self.acc.at[(color,) + where + (h, slice(None), into)], dst_ref=out.at[rows, cols],
                    send_sem=sems[0].at[color, n], recv_sem=sems[1].at[color, n], device_id={"pp": self.partner}, device_id_type=MESH)))
        return copies


def give_finals(red, outs, sems):
    for dst, src, copy in red.finals(outs, sems):
        copy.start()
        dst[...] = src[...]


def end_finals(red, outs, sems):
    for _, _, copy in red.finals(outs, sems):
        copy.wait_send()
        copy.wait_recv()


def reduce_kernel(up_ref, down_ref, qkv_ref, proj_ref, oup, odown, oqkv, oproj,
                  acc, peer, t1a, t2a, t1b, t2b, t1c, t2c,
                  load_sem, psend_sem, precv_sem, send_sem, recv_sem, fsend_sem, frecv_sem):
    refs, outs = (up_ref, down_ref, qkv_ref, proj_ref), (oup, odown, oqkv, oproj)
    red = Reducer(acc, ((t1a, t2a), (t1b, t2b), (t1c, t2c)), (send_sem, recv_sem))
    swap_sems, final_sems = (psend_sem, precv_sem), (fsend_sem, frecv_sem)
    for pos in range(4):
        for color in range(3):
            for copy in red.loads(refs, load_sem, color, pos):
                copy.start()
    enter(red.me, red.partner)
    for pos in range(4):
        for color in range(3):
            for copy in red.swaps(refs, peer, swap_sems, color, pos):
                copy.start()
    for pos in range(4):
        red.swapped(refs, peer, load_sem, swap_sems, pos)
    for phase in range(3):
        if phase:
            red.all_first(phase)
        red.second(phase)
        red.third(phase)
        red.fourth(phase)
    give_finals(red, outs, final_sems)
    end_finals(red, outs, final_sems)
    for phase in range(3):
        red.drain(phase)
    for pos in range(4):
        for color in range(3):
            for copy in red.swaps(refs, peer, swap_sems, color, pos):
                copy.wait_send()


def grad_views(grads):
    g_qkv, g_proj, g_up, g_down = grads
    return [g.reshape(4, 4, 4, g.shape[0] // 64, g.shape[1]) for g in (g_up, g_down, g_qkv, g_proj)]


VMEM, DMA = pltpu.VMEM, pltpu.SemaphoreType.DMA
SWAP_SCRATCH = [VMEM((3, 4, 4, 4, 2, 8, 512), F32), VMEM((3, 4, 4, 4, 2, 8, 512), F32)]
PHASE_SCRATCH = [
    [VMEM((3, 2, 4, 4, 8, 512), F32), VMEM((3, 2, 2, 4, 4, 8, 512), F32)],
    [VMEM((3, 2, 4, 8, 512), F32), VMEM((3, 2, 2, 4, 8, 512), F32)],
    [VMEM((3, 2, 8, 512), F32), VMEM((3, 2, 2, 8, 512), F32)],
]
SWAP_SEMS = [DMA((3, 4, 3)), DMA((3, 4, 3)), DMA((3, 4, 3))]
PHASE_SEMS = lambda n: [DMA((3, n, 6)), DMA((3, n, 6))]
FINAL_SEMS = [DMA((3, 3)), DMA((3, 3))]


def reduce_grads(grads, which):
    args = grad_views(grads)
    outs = pl.pallas_call(
        reduce_kernel,
        in_specs=[pl.BlockSpec(memory_space=pl.ANY)] * 4,
        out_specs=[pl.BlockSpec(memory_space=VMEM)] * 4,
        out_shape=[jax.ShapeDtypeStruct(a.shape[3:], F32) for a in args],
        scratch_shapes=SWAP_SCRATCH + sum(PHASE_SCRATCH, []) + SWAP_SEMS + PHASE_SEMS(3) + FINAL_SEMS,
        compiler_params=pltpu.CompilerParams(collective_id=1 + which, has_side_effects=True, vmem_limit_bytes=30 << 20),
        name="reduce_grads",
    )(*args)
    return outs[2], outs[3], outs[0], outs[1]


def ffn_bwd_kernel(tile, carry, *refs):
    ge_ref, up_ref, ct_ref, n2_ref, mid_ref, at_ref, wd_ref, wu_ref, wp_ref = refs[:9]
    refs = refs[9:]
    step = pl.program_id(0)
    last = pl.num_programs(0) - 1
    at = lambda k, f: pl.when(step == k)(f)
    if carry:
        grads, refs = refs[:4], refs[4:]
        reduced = refs[5]
        acc_g, peer, near, final, load_sem, psend, precv, send_sem, recv_sem = refs[8:]
        red = Reducer(acc_g, ((near, final),), (send_sem, recv_sem))
        swap_sems = (psend, precv)
    gd_ref, gu_ref, gp_ref, cm_ref, ca_ref = refs[:5]
    acc, ctu = refs[6:8] if carry else refs[5:7]

    def every(what):
        for pos in range(4):
            for color in range(3):
                for copy in what(color, pos):
                    yield copy

    def begin():
        for copy in every(lambda color, pos: red.loads(grads, load_sem, color, pos)):
            copy.start()
        enter(red.me, red.partner)
        for copy in every(lambda color, pos: red.swaps(grads, peer, swap_sems, color, pos)):
            copy.start()

    def finish():
        red.fourth(0, reduced)
        red.drain(0)
        for copy in every(lambda color, pos: red.swaps(grads, peer, swap_sems, color, pos)):
            copy.wait_send()

    def swapped(*positions):
        for pos in positions:
            red.swapped(grads, peer, load_sem, swap_sems, pos)

    def carried_step():
        if carry:
            todo = {
                0: begin,
                1: lambda: swapped(0, 1, 2, 3),
                2: lambda: red.second(0),
                3: lambda: red.third(0),
            }
            for k, f in todo.items():
                at(k, f)

    carried_step()
    chunks = range(0, ct_ref.shape[0], tile)
    for m in chunks:
        rows = slice(m, m + tile)
        cg = dot_nt(ct_ref[rows, :], wd_ref[...]).astype(BF).astype(F32)
        ctu[rows, :] = gelu_pull(up_ref[rows, :].astype(F32), cg).astype(BF)
    gd_ref[...] = dot_tn(ge_ref[...], ct_ref[...])
    gu_ref[...] = dot_tn(n2_ref[...], ctu[...])
    part = dot_nt(ctu[...], wu_ref[...])

    @pl.when(step == 0)
    def _():
        acc[...] = part

    @pl.when(step > 0)
    def _():
        acc[...] += part

    @pl.when(step == last)
    def _():
        pulled = rms_pull(mid_ref[...].astype(F32), acc[...].astype(BF).astype(F32))
        cm_ref[...] = (ct_ref[...].astype(F32) + pulled).astype(BF)
        ca_ref[...] = dot_nt(cm_ref[...], wp_ref[...]).astype(BF)
        gp_ref[...] = dot_tn(at_ref[...], cm_ref[...])

    if carry:
        at(last, finish)


def ffn_bwd(gelu, up, ct, normed2, mid, attn, w_down, w_up, w_proj, layer, tile, carried):
    tokens, d = ct.shape
    ff = gelu.shape[1]
    part = 512
    act = whole((tokens, d))
    cols = pl.BlockSpec((tokens, part), lambda i: (0, i))
    in_specs = [cols, cols, act, act, act, act,
                pl.BlockSpec((None, part, d), lambda i: (layer, i, 0)), pl.BlockSpec((None, d, part), lambda i: (layer, 0, i)), whole((d, d), layer)]
    out_specs = [pl.BlockSpec((part, d), lambda i: (i, 0)), pl.BlockSpec((d, part), lambda i: (0, i)), whole((d, d)), act, act]
    out_shape = [jax.ShapeDtypeStruct((ff, d), F32), jax.ShapeDtypeStruct((d, ff), F32), jax.ShapeDtypeStruct((d, d), F32),
                 jax.ShapeDtypeStruct((tokens, d), BF), jax.ShapeDtypeStruct((tokens, d), BF)]
    scratch = [VMEM((tokens, d), F32), VMEM((tokens, part), BF)]
    params = dict(vmem_limit_bytes=50 << 20)
    args = (gelu, up, ct, normed2, mid, attn, w_down, w_up, w_proj)
    carry = carried is not None
    if carry:
        args = args + tuple(grad_views(carried))
        in_specs = in_specs + [pl.BlockSpec(memory_space=pl.ANY)] * 4
        out_specs = out_specs + [whole((3, 4, 4, 2, 8, 512))]
        out_shape = out_shape + [jax.ShapeDtypeStruct((3, 4, 4, 2, 8, 512), F32)]
        scratch = scratch + SWAP_SCRATCH + PHASE_SCRATCH[0] + SWAP_SEMS + PHASE_SEMS(1)
        params = dict(vmem_limit_bytes=62 << 20, collective_id=2, has_side_effects=True)
    return pl.pallas_call(
        functools.partial(ffn_bwd_kernel, tile, carry),
        grid=(ff // part,), in_specs=in_specs, out_specs=out_specs, out_shape=out_shape, scratch_shapes=scratch,
        compiler_params=pltpu.CompilerParams(**params),
        name="ffn_bwd_carry" if carry else "ffn_bwd",
    )(*args)


def attn_carry_kernel(scale, width, q_ref, k_ref, v_ref, do_ref, acc_hbm, dqkv_ref, *rest):
    results, (acc_ref, sup, sdown, sqkv, sproj, t1b, t2b, t1c, t2c, load_sem, send_sem, recv_sem, fsend_sem, frecv_sem) = rest[:4], rest[4:]
    steps = pl.num_programs(1)
    step = pl.program_id(0) * steps + pl.program_id(1)
    red = Reducer(acc_ref, (None, (t1b, t2b), (t1c, t2c)), (send_sem, recv_sem), start=1)
    outs, sems = (sup, sdown, sqkv, sproj), (fsend_sem, frecv_sem)

    def begin():
        load = pltpu.make_async_copy(acc_hbm, acc_ref, load_sem)
        load.start()
        enter(red.me, red.partner)
        load.wait()
        red.all_first(1)

    def turn():
        red.fourth(1)
        red.all_first(2)

    def close():
        red.fourth(2)
        give_finals(red, outs, sems)

    def third_second():
        red.third(1)

    todo = {0: begin, 2: lambda: red.second(1), 3: third_second, 4: turn, 5: lambda: red.second(2), 6: lambda: red.third(2), 7: close}
    for k, f in todo.items():
        pl.when(step == k)(f)
    attn_bwd_kernel(scale, width, q_ref, k_ref, v_ref, do_ref, dqkv_ref)

    @pl.when(step == pl.num_programs(0) * steps - 1)
    def _():
        end_finals(red, outs, sems)
        red.drain(1)
        red.drain(2)
        for result, out in zip(results, outs):
            result[...] = out[...]


def attn_bwd(qkv, do, seq, scale, carried):
    tokens, width = qkv.shape[0], qkv.shape[1] // 3
    steps = width // 256
    spec = lambda off: pl.BlockSpec((seq, 256), lambda b, j: (b, off + j))
    in_specs = [spec(0), spec(steps), spec(2 * steps), spec(0)]
    out_specs = [pl.BlockSpec((seq, 3 * width), lambda b, j: (b, 0))]
    out_shape = [jax.ShapeDtypeStruct((tokens, 3 * width), BF)]
    args, scratch, params, kernel = (qkv, qkv, qkv, do), [], {}, attn_bwd_kernel
    if carried is not None:
        args = args + (carried,)
        kernel = attn_carry_kernel
        in_specs = in_specs + [pl.BlockSpec(memory_space=pl.ANY)]
        shapes = ((8, 2048), (32, 512), (8, 1536), (8, 512))
        out_specs = out_specs + [whole(s) for s in shapes]
        out_shape = out_shape + [jax.ShapeDtypeStruct(s, F32) for s in shapes]
        scratch = [VMEM(s, F32) for s in (carried.shape,) + shapes] + PHASE_SCRATCH[1] + PHASE_SCRATCH[2] + [DMA] + PHASE_SEMS(2) + FINAL_SEMS
        params = dict(collective_id=3, has_side_effects=True, vmem_limit_bytes=50 << 20)
    return pl.pallas_call(
        functools.partial(kernel, scale, width),
        grid=(tokens // seq, steps), in_specs=in_specs, out_specs=out_specs, out_shape=out_shape, scratch_shapes=scratch,
        compiler_params=pltpu.CompilerParams(**params),
        name="attn_bwd" if carried is None else "attn_bwd_carry",
    )(*args)


def layer_forward(hidden, weights, layer, seq, scale):
    w_qkv, w_proj, w_up, w_down = weights
    normed, qkv = pre_attn(hidden, w_qkv, layer, seq)
    attn = attn_fwd(qkv, seq, scale)
    mid, normed2, up, gelu, out = post_attn(hidden, attn, w_proj, w_up, w_down, layer, seq)
    return out, (hidden, normed, qkv, attn, mid, normed2, up, gelu)


def layer_backward(saved, ct_out, weights, layer, seq, scale, carried):
    w_qkv, w_proj, w_up, w_down = weights
    hidden, normed, qkv, attn, mid, normed2, up, gelu = saved
    res = ffn_bwd(gelu, up, ct_out, normed2, mid, attn, w_down, w_up, w_proj, layer, seq, carried)
    g_down, g_up, g_proj, ct_mid, ct_attn = res[:5]
    res = attn_bwd(qkv, ct_attn, seq, scale, res[5] if carried is not None else None)
    ct_qkv = res[0]
    g_qkv = dot_tn(normed, ct_qkv)
    grads = (g_qkv, g_proj, g_up, g_down)
    if carried is not None:
        return grads, (res[3], res[4], res[1], res[2])
    ct_norm = dot_nt(ct_qkv, w_qkv[layer]).astype(BF)
    ct_hidden = (ct_mid.astype(F32) + rms_pull(hidden.astype(F32), ct_norm.astype(F32))).astype(BF)
    return grads, ct_hidden


def solution(mesh):
    stages = mesh.shape['pp']
    grid = Mesh(mesh.devices.reshape(2, 4, 4, 4), ("pp", "z", "y", "x"))
    dp = ("z", "y", "x")
    swap = [(0, 1), (1, 0)]

    def device_step(act_in, loss_seed, w_qkv, w_proj, w_up, w_down):
        micro, _, seq, d = act_in.shape
        mine = micro // 2
        pp = lax.axis_index('pp')
        heads3, hd = w_qkv.shape[2:]
        scale = hd ** -0.5

        full = gather_weights(*(w.reshape(w.shape[1], -1) for w in (w_qkv, w_proj, w_up, w_down)))
        act = lax.dynamic_slice_in_dim(act_in, pp * mine, mine, 0).reshape(mine * seq, d)
        seed = lax.dynamic_slice_in_dim(loss_seed, pp * mine, mine, 0).reshape(mine * seq, d)
        h1, saved0 = layer_forward(act, full, 0, seq, scale)
        h2, saved1 = layer_forward(h1, full, 1, seq, scale)

        out4 = h2.reshape(mine, 1, seq, d)
        half = seq // 2
        keep = lax.dynamic_slice_in_dim(out4, pp * half, half, 2)
        give = lax.dynamic_slice_in_dim(out4, (1 - pp) * half, half, 2)
        got = lax.ppermute(give, 'pp', swap)
        act_out = jnp.concatenate([jnp.where(pp == 0, keep, got), jnp.where(pp == 0, got, keep)], axis=0)

        grads1, ct1 = layer_backward(saved1, seed, full, 1, seq, scale, None)
        grads0, red1 = layer_backward(saved0, ct1, full, 0, seq, scale, grads1)
        red0 = reduce_grads(grads0, 0)
        outs = [jnp.where(pp == 0, a, b) for a, b in zip(red0, red1)]
        return tuple(o.reshape(w.shape) for o, w in zip(outs, (w_qkv, w_proj, w_up, w_down))) + (act_out,)

    weight_spec = P('pp', dp)
    act_spec = P(None, dp)
    return jax.shard_map(device_step, mesh=grid, in_specs=(act_spec, act_spec) + (weight_spec,) * 4, out_specs=(weight_spec,) * 4 + (P(None, dp, 'pp'),), check_vma=False)
```

```python
import functools

import jax
import jax.numpy as jnp
from jax import lax
from jax.experimental import pallas as pl
from jax.experimental.pallas import tpu as pltpu
from jax.sharding import Mesh
from jax.sharding import PartitionSpec as P

NORM_EPS = 1e-6
BF = jnp.bfloat16
F32 = jnp.float32


def rms_norm(hidden):
    return hidden * lax.rsqrt(jnp.mean(hidden * hidden, axis=-1, keepdims=True) + NORM_EPS)


def dot(a, b):
    return lax.dot_general(a, b, (((1,), (0,)), ((), ())), preferred_element_type=F32)


def dot_nt(a, b):
    return lax.dot_general(a, b, (((1,), (1,)), ((), ())), preferred_element_type=F32)


def dot_tn(a, b):
    return lax.dot_general(a, b, (((0,), (0,)), ((), ())), preferred_element_type=F32)


LOG2E = 1.4426950408889634
GELU_A = 0.7978845608028654
GELU_B = GELU_A * 0.044715


def split_heads(refs, count):
    low = lax.broadcasted_iota(jnp.int32, (refs[0].shape[0], 128), 1) < 64
    zero = jnp.zeros((refs[0].shape[0], 128), BF)
    heads = []
    for h in range(count):
        keep = low if h % 2 == 0 else jnp.logical_not(low)
        lanes = slice((h // 2) * 128, (h // 2) * 128 + 128)
        heads.append([(r[:, lanes], jnp.where(keep, r[:, lanes], zero)) for r in refs])
    return heads


def causal_mask(n):
    return lax.broadcasted_iota(jnp.int32, (n, n), 0) >= lax.broadcasted_iota(jnp.int32, (n, n), 1)


def softmax_rows(s, keep, scale):
    s = jnp.where(keep, s, -1e30)
    e = jnp.exp2((s - jnp.max(s, axis=-1, keepdims=True)) * (scale * LOG2E))
    return e * (1.0 / jnp.sum(e, axis=-1, keepdims=True))


def row_blocks(seq, parts):
    return parts if seq == parts[-1][1] else ((0, seq),)


def attn_fwd_kernel(scale, q_ref, k_ref, v_ref, o_ref):
    seq, lanes = q_ref.shape
    count = lanes // 64
    blocks = row_blocks(seq, ((0, 128), (128, 256), (256, 384)))
    keep = causal_mask(seq)
    heads = split_heads((q_ref, k_ref, v_ref), count)
    scores = [[dot_nt(q[0][a:b], k[1][:b]) for a, b in blocks] for q, k, v in heads]
    probs = [[softmax_rows(s, keep[a:b, :b], scale).astype(BF) for (a, b), s in zip(blocks, row)] for row in scores]
    for h in range(0, count, 2):
        for n, (a, b) in enumerate(blocks):
            pair = dot(probs[h][n], heads[h][2][1][:b]) + dot(probs[h + 1][n], heads[h + 1][2][1][:b])
            o_ref[a:b, (h // 2) * 128:(h // 2) * 128 + 128] = pair.astype(BF)


def attn_bwd_kernel(scale, width, q_ref, k_ref, v_ref, do_ref, dqkv_ref):
    seq, lanes = q_ref.shape
    count = lanes // 64
    blocks = row_blocks(seq, ((0, 256), (256, 384)))
    keep = causal_mask(seq)
    base = pl.program_id(1) * lanes
    heads = split_heads((q_ref, k_ref, v_ref, do_ref), count)
    firsts = [[(dot_nt(q[0][a:b], k[1][:b]), dot_nt(do[0][a:b], v[1][:b])) for a, b in blocks] for q, k, v, do in heads]
    work = []
    for row in firsts:
        done = []
        for (a, b), (s, dp) in zip(blocks, row):
            p = softmax_rows(s, keep[a:b, :b], scale)
            dp = dp.astype(BF).astype(F32)
            delta = jnp.sum(dp * p, axis=-1, keepdims=True)
            done.append((p.astype(BF), (p * (dp - delta) * scale).astype(BF)))
        work.append(done)
    total = lambda terms: functools.reduce(lambda x, y: x + y, terms)
    for j in range(count // 2):
        pair = (2 * j, 2 * j + 1)
        cols = [pl.ds(pl.multiple_of(base + j * 128 + i * width, 128), 128) for i in range(3)]
        for n, (a, b) in enumerate(blocks):
            dqkv_ref[a:b, cols[0]] = total([dot(work[h][n][1], heads[h][1][1][:b]) for h in pair]).astype(BF)
        for i, (_, hi) in enumerate(blocks):
            lo = blocks[i - 1][1] if i else 0
            later = [(n, a, b, h) for n, (a, b) in enumerate(blocks) if n >= i for h in pair]
            dqkv_ref[lo:hi, cols[1]] = total([dot_tn(work[h][n][1][:, lo:hi], heads[h][0][1][a:b]) for n, a, b, h in later]).astype(BF)
            dqkv_ref[lo:hi, cols[2]] = total([dot_tn(work[h][n][0][:, lo:hi], heads[h][3][1][a:b]) for n, a, b, h in later]).astype(BF)


def attn_fwd(qkv, seq, scale):
    tokens, width = qkv.shape[0], qkv.shape[1] // 3
    spec = lambda off: pl.BlockSpec((seq, width // 2), lambda b, j: (b, off + j))
    return pl.pallas_call(
        functools.partial(attn_fwd_kernel, scale),
        grid=(tokens // seq, 2),
        in_specs=[spec(0), spec(2), spec(4)],
        out_specs=spec(0),
        out_shape=jax.ShapeDtypeStruct((tokens, width), BF),
        name="attn_fwd",
    )(qkv, qkv, qkv)


def pre_kernel(_, h_ref, w_ref, n_ref, qkv_ref):
    normed = rms_norm(h_ref[...].astype(F32)).astype(BF)
    n_ref[...] = normed
    qkv_ref[...] = dot(normed, w_ref[...]).astype(BF)


def whole(shape, layer=None):
    block = shape if layer is None else (None,) + shape
    index = (0,) * len(shape) if layer is None else (layer,) + (0,) * len(shape)
    return pl.BlockSpec(block, lambda *_: index, pipeline_mode=pl.Buffered(1))


def rows_at(tile, n, shifted=False):
    return pl.BlockSpec((tile, n), lambda i, first: (i + first[0] if shifted else i, 0))


def pre_attn(hidden, first, tokens, w_qkv, layer, tile):
    d = hidden.shape[1]
    cols = w_qkv.shape[2]
    return pl.pallas_call(
        pre_kernel,
        grid_spec=pltpu.PrefetchScalarGridSpec(
            num_scalar_prefetch=1, grid=(tokens // tile,),
            in_specs=[rows_at(tile, d, True), whole((d, cols), layer)],
            out_specs=[rows_at(tile, d), rows_at(tile, cols)]),
        out_shape=[jax.ShapeDtypeStruct((tokens, d), BF), jax.ShapeDtypeStruct((tokens, cols), BF)],
        name="pre_attn",
    )(first, hidden, w_qkv)


def post_kernel(_, h_ref, a_ref, wp_ref, wu_ref, wd_ref, mid_ref, n2_ref, up_ref, ge_ref, out_ref):
    mid = (h_ref[...].astype(F32) + dot(a_ref[...], wp_ref[...])).astype(BF)
    mid_ref[...] = mid
    mid_f32 = mid.astype(F32)
    n2 = rms_norm(mid_f32).astype(BF)
    n2_ref[...] = n2
    ff = wu_ref.shape[1]

    def chunk(c, _):
        cols = pl.ds(pl.multiple_of(c * 512, 512), 512)
        up = dot(n2_ref[...], wu_ref[:, cols]).astype(BF)
        up_ref[:, cols] = up
        u = up.astype(F32)
        t = jnp.tanh(u * (GELU_A + GELU_B * (u * u)))
        ge_ref[:, cols] = (u * (0.5 * t + 0.5)).astype(BF)
        return 0

    lax.fori_loop(0, ff // 512, chunk, 0)
    out_ref[...] = (mid_f32 + dot(ge_ref[...], wd_ref[...])).astype(BF)


def post_attn(hidden, first, attn, w_proj, w_up, w_down, layer, tile):
    tokens, d = attn.shape
    ff = w_up.shape[2]
    sizes = (d, d, ff, ff, d)
    return pl.pallas_call(
        post_kernel,
        grid_spec=pltpu.PrefetchScalarGridSpec(
            num_scalar_prefetch=1, grid=(tokens // tile,),
            in_specs=[rows_at(tile, d, True), rows_at(tile, d), whole((d, d), layer), whole((d, ff), layer), whole((ff, d), layer)],
            out_specs=[rows_at(tile, n) for n in sizes]),
        out_shape=[jax.ShapeDtypeStruct((tokens, n), BF) for n in sizes],
        name="post_attn",
    )(first, hidden, attn, w_proj, w_up, w_down)


def gelu_pull(u, g):
    u2 = u * u
    s = 0.5 * jnp.tanh(u * (GELU_A + GELU_B * u2)) + 0.5
    return g * (s + (s - s * s) * (u * (2 * GELU_A + (6 * GELU_B) * u2)))


def rms_pull(m, g):
    r = lax.rsqrt(jnp.mean(m * m, axis=-1, keepdims=True) + NORM_EPS)
    return g * r - m * (r * r * r * jnp.mean(g * m, axis=-1, keepdims=True))


MESH = pl.DeviceIdType.MESH
AXES = ("z", "y", "x")
GATHER_ORDER = ((2, 1, 0), (0, 2, 1), (1, 0, 2))
REDUCE_ORDER = ((0, 1, 2), (1, 2, 0), (2, 0, 1))


def step_coord(pos, by):
    return lax.rem(pos + by, 4)


def neighbour(me, axis, by):
    return {AXES[axis]: step_coord(me[axis], by)}


def enter(me, partner):
    barrier = pltpu.get_barrier_semaphore()
    for axis in range(3):
        for by in (1, 3):
            pl.semaphore_signal(barrier, inc=1, device_id=neighbour(me, axis, by), device_id_type=MESH)
    pl.semaphore_signal(barrier, inc=1, device_id={"pp": partner}, device_id_type=MESH)
    pl.semaphore_wait(barrier, 7)


def remote(src, dst, send, recv, where):
    copy = pltpu.make_async_remote_copy(src_ref=src, dst_ref=dst, send_sem=send, recv_sem=recv, device_id=where, device_id_type=MESH)
    copy.start()
    return copy


def gather_kernel(up_ref, down_ref, qkv_ref, proj_ref, *rest):
    results, bufs, (local_sem, send_sem, recv_sem, psend_sem, precv_sem, out_sem) = rest[:4], rest[4:8], rest[8:]
    pp = lax.axis_index("pp")
    partner = 1 - pp
    me = tuple(lax.axis_index(a) for a in AXES)
    sources = (up_ref, down_ref, qkv_ref, proj_ref)
    groups = (0, 1, 2, 2)

    def region(base, n, phase, by, half, layer):
        order = GATHER_ORDER[groups[n]]
        idx = [None, None, None]
        for later, axis in enumerate(order):
            idx[axis] = slice(None) if later < phase else step_coord(me[axis], by if later == phase else 0)
        rows, cols = base[n].shape[-2:]
        tail = (slice(None), slice(None))
        if half is not None and rows > 8:
            tail = (pl.ds(half * (rows // 2), rows // 2), slice(None))
        elif half is not None:
            tail = (slice(None), pl.ds(half * (cols // 2), cols // 2))
        return base[n].at[(layer,) + tuple(idx) + tail]

    own = [pltpu.make_async_copy(src, bufs[n].at[(pp,) + me], local_sem.at[n]) for n, src in enumerate(sources)]
    for copy in own:
        copy.start()
    enter(me, partner)
    for copy in own:
        copy.wait()

    sends, partners, locals_ = [], [], []

    def put_out(n, slot, by, half, layer, side):
        copy = pltpu.make_async_copy(region(bufs, n, 2, by, half, layer), region(results, n, 2, by, half, layer), out_sem.at[n, slot, side])
        copy.start()
        locals_.append(copy)

    def ready(n, slot, by, half):
        ref = region(bufs, n, 2, by, half, pp)
        copy = remote(ref, ref, psend_sem.at[n, slot], precv_sem.at[n, slot], {"pp": partner})
        partners.append((copy, n, slot, by, half))
        put_out(n, slot, by, half, pp, 0)

    def send(n, phase, slot, by, half, to):
        axis = GATHER_ORDER[groups[n]][phase]
        ref = region(bufs, n, phase, by, half, pp)
        sends.append(remote(ref, ref, send_sem.at[n, phase, slot], recv_sem.at[n, phase, slot], neighbour(me, axis, to)))

    def arrived(n, phase, slot, by, half):
        ref = region(bufs, n, phase, by, half, pp)
        pltpu.make_async_copy(ref, ref, recv_sem.at[n, phase, slot]).wait()
        if phase == 2:
            ready(n, slot + 1, by, half)

    for phase in range(3):
        for n in range(4):
            send(n, phase, 0, 0, 0, 1)
            send(n, phase, 1, 0, 1, 3)
        for n in range(4):
            send(n, phase, 2, 0, 1, 1)
            send(n, phase, 3, 0, 0, 3)
            if phase == 2:
                ready(n, 0, 0, None)
        for n in range(4):
            arrived(n, phase, 0, 3, 0)
            send(n, phase, 4, 3, 0, 1)
            arrived(n, phase, 1, 1, 1)
            send(n, phase, 5, 1, 1, 3)
        for n in range(4):
            arrived(n, phase, 2, 3, 1)
            arrived(n, phase, 3, 1, 0)
        for n in range(4):
            arrived(n, phase, 4, 2, 0)
            arrived(n, phase, 5, 2, 1)
    for copy, n, slot, by, half in partners:
        copy.wait_recv()
        put_out(n, slot, by, half, partner, 1)
    for copy in sends:
        copy.wait_send()
    for copy, *_ in partners:
        copy.wait_send()
    for copy in locals_:
        copy.wait()


def gather_weights(w_qkv, w_proj, w_up, w_down):
    vmem = pl.BlockSpec(memory_space=pltpu.VMEM)
    shape = lambda w: (2, 4, 4, 4) + w.shape
    dma = pltpu.SemaphoreType.DMA
    args = (w_up, w_down, w_qkv, w_proj)
    outs = pl.pallas_call(
        gather_kernel,
        in_specs=[vmem] * 4,
        out_specs=[pl.BlockSpec(memory_space=pltpu.HBM)] * 4,
        out_shape=[jax.ShapeDtypeStruct(shape(w), BF) for w in args],
        scratch_shapes=[pltpu.VMEM(shape(w), BF) for w in args] + [dma((4,)), dma((4, 3, 6)), dma((4, 3, 6)), dma((4, 7)), dma((4, 7)), dma((4, 7, 2))],
        compiler_params=pltpu.CompilerParams(collective_id=0, has_side_effects=True, vmem_limit_bytes=62 << 20),
        name="gather_weights",
    )(*args)
    flat = [o.reshape(2, -1, o.shape[-1]) for o in outs]
    return flat[2], flat[3], flat[0], flat[1]


REDUCE_OFFSETS = (2, 1, 3, 0)


def reduce_pieces(refs, color, core):
    up_ref, down_ref, qkv_ref, proj_ref = refs
    if color == 0:
        return [(up_ref, pl.ds(0, 8), pl.ds(pl.multiple_of(core * 1024 + h * 512, 128), 512), h, pl.ds(0, 512)) for h in range(2)]
    if color == 1:
        return [(down_ref, pl.ds(pl.multiple_of(core * 16 + h * 8, 8), 8), pl.ds(0, 512), h, pl.ds(0, 512)) for h in range(2)]
    return [
        (qkv_ref, pl.ds(0, 8), pl.ds(pl.multiple_of(core * 768, 128), 512), 0, pl.ds(0, 512)),
        (qkv_ref, pl.ds(0, 8), pl.ds(pl.multiple_of(core * 768 + 512, 128), 256), 1, pl.ds(0, 256)),
        (proj_ref, pl.ds(0, 8), pl.ds(pl.multiple_of(core * 256, 128), 256), 1, pl.ds(256, 256)),
    ]


def add_block(out, dst, src):
    if len(dst.shape) < 4:
        out[...] = dst[...] + src[...]
        return

    def body(i, _):
        out[i] = dst[i] + src[i]
        return 0

    lax.fori_loop(0, dst.shape[0], body, 0)


class Reducer:
    def __init__(self, acc, slots, sems, start=0):
        self.pp = lax.axis_index("pp")
        self.partner = 1 - self.pp
        self.me = tuple(lax.axis_index(a) for a in AXES)
        self.acc, self.slots, self.start = acc, slots, start
        self.send_sem, self.recv_sem = sems

    def lead(self, color, phase, where):
        order = REDUCE_ORDER[color]
        idx = [None, None, None]
        for later, axis in enumerate(order):
            idx[axis] = self.me[axis] if later < phase else (where if later == phase else slice(None))
        return tuple(v for axis, v in enumerate(idx) if order.index(axis) >= self.start)

    def place(self, color, phase, by):
        return step_coord(self.me[REDUCE_ORDER[color][phase]], by)

    def loads(self, refs, sem, color, pos):
        where = self.lead(color, 0, self.place(color, 0, REDUCE_OFFSETS[pos]))
        return [
            pltpu.make_async_copy(ref.at[where + (rows, cols)], self.acc.at[(color,) + where + (h, slice(None), into)], sem.at[color, pos, n])
            for n, (ref, rows, cols, h, into) in enumerate(reduce_pieces(refs, color, self.pp))
        ]

    def swaps(self, refs, peer, sems, color, pos):
        where = self.lead(color, 0, self.place(color, 0, REDUCE_OFFSETS[pos]))
        return [
            pltpu.make_async_remote_copy(
                src_ref=ref.at[where + (rows, cols)], dst_ref=peer.at[(color,) + where + (h, slice(None), into)],
                send_sem=sems[0].at[color, pos, n], recv_sem=sems[1].at[color, pos, n], device_id={"pp": self.partner}, device_id_type=MESH)
            for n, (ref, rows, cols, h, into) in enumerate(reduce_pieces(refs, color, self.partner))
        ]

    def part(self, color, phase, by, half):
        return self.acc.at[(color,) + self.lead(color, phase, self.place(color, phase, by)) + (half,)]

    def near(self, color, phase, side):
        return self.slots[phase][0].at[color, side]

    def final(self, color, phase, side, half):
        return self.slots[phase][1].at[color, side, half]

    def copy(self, color, phase, n):
        part, near, final = self.part, self.near, self.final
        plan = (
            (part(color, phase, 2, 0), near(color, phase, 0), 1),
            (part(color, phase, 2, 1), near(color, phase, 1), 3),
            (part(color, phase, 1, 1), final(color, phase, 0, 1), 1),
            (part(color, phase, 3, 0), final(color, phase, 1, 0), 3),
            (part(color, phase, 1, 0), final(color, phase, 0, 0), 1),
            (part(color, phase, 3, 1), final(color, phase, 1, 1), 3),
        )
        k = phase - self.start
        src, dst, by = plan[n]
        return pltpu.make_async_remote_copy(
            src_ref=src, dst_ref=dst, send_sem=self.send_sem.at[color, k, n], recv_sem=self.recv_sem.at[color, k, n],
            device_id=neighbour(self.me, REDUCE_ORDER[color][phase], by), device_id_type=MESH)

    def first_sends(self, color, phase, by):
        for n in {2: (0, 1), 1: (2,), 3: (3,), 0: ()}[by]:
            self.copy(color, phase, n).start()

    def start_swaps(self, refs, peer, swap_sems, pos):
        if pos < 4:
            for color in range(3):
                for copy in self.swaps(refs, peer, swap_sems, color, pos):
                    copy.start()

    def swapped(self, refs, peer, load_sem, swap_sems, pos):
        by = REDUCE_OFFSETS[pos]
        for color in range(3):
            for copy in self.loads(refs, load_sem, color, pos):
                copy.wait()
            for copy in self.swaps(refs, peer, swap_sems, color, pos):
                copy.wait_recv()
        self.start_swaps(refs, peer, swap_sems, pos + 1)
        for color in range(3):
            block = self.acc.at[(color,) + self.lead(color, 0, self.place(color, 0, by))]
            add_block(block, block, peer.at[(color,) + self.lead(color, 0, self.place(color, 0, by))])
            self.first_sends(color, 0, by)

    def all_first(self, phase):
        for by in (2, 1, 3):
            for color in range(3):
                self.first_sends(color, phase, by)

    def second(self, phase):
        for color in range(3):
            for n, by, half in ((0, 1, 0), (1, 3, 1)):
                self.copy(color, phase, n).wait_recv()
                dst = self.part(color, phase, by, half)
                add_block(dst, dst, self.near(color, phase, n))
                self.copy(color, phase, n + 4).start()

    def third(self, phase):
        for color in range(3):
            for n, side, half in ((2, 0, 1), (3, 1, 0)):
                self.copy(color, phase, n).wait_recv()
                dst = self.part(color, phase, 0, half)
                add_block(dst, dst, self.final(color, phase, side, half))

    def fourth(self, phase, out=None):
        for color in range(3):
            for n, side, half in ((4, 0, 0), (5, 1, 1)):
                self.copy(color, phase, n).wait_recv()
                dst = self.part(color, phase, 0, half)
                add_block(dst if out is None else out.at[color, :, :, half], dst, self.final(color, phase, side, half))

    def drain(self, phase):
        for color in range(3):
            for n in range(6):
                self.copy(color, phase, n).wait_send()

    def finals(self, outs, sems):
        copies = []
        for color in range(3):
            for n, (out, rows, cols, h, into) in enumerate(reduce_pieces(outs, color, self.pp)):
                where = self.lead(color, 3, None)
                copies.append((out.at[rows, cols], self.acc.at[(color,) + where + (h, slice(None), into)], pltpu.make_async_remote_copy(
                    src_ref=self.acc.at[(color,) + where + (h, slice(None), into)], dst_ref=out.at[rows, cols],
                    send_sem=sems[0].at[color, n], recv_sem=sems[1].at[color, n], device_id={"pp": self.partner}, device_id_type=MESH)))
        return copies


def give_finals(red, outs, sems):
    for dst, src, copy in red.finals(outs, sems):
        copy.start()
        dst[...] = src[...]


def end_finals(red, outs, sems):
    for _, _, copy in red.finals(outs, sems):
        copy.wait_send()
        copy.wait_recv()


def reduce_kernel(up_ref, down_ref, qkv_ref, proj_ref, oup, odown, oqkv, oproj,
                  acc, peer, t1a, t2a, t1b, t2b, t1c, t2c,
                  load_sem, psend_sem, precv_sem, send_sem, recv_sem, fsend_sem, frecv_sem):
    refs, outs = (up_ref, down_ref, qkv_ref, proj_ref), (oup, odown, oqkv, oproj)
    red = Reducer(acc, ((t1a, t2a), (t1b, t2b), (t1c, t2c)), (send_sem, recv_sem))
    swap_sems, final_sems = (psend_sem, precv_sem), (fsend_sem, frecv_sem)
    for pos in range(4):
        for color in range(3):
            for copy in red.loads(refs, load_sem, color, pos):
                copy.start()
    enter(red.me, red.partner)
    red.start_swaps(refs, peer, swap_sems, 0)
    for pos in range(4):
        red.swapped(refs, peer, load_sem, swap_sems, pos)
    for phase in range(3):
        if phase:
            red.all_first(phase)
        red.second(phase)
        red.third(phase)
        red.fourth(phase)
    give_finals(red, outs, final_sems)
    end_finals(red, outs, final_sems)
    for phase in range(3):
        red.drain(phase)
    for pos in range(4):
        for color in range(3):
            for copy in red.swaps(refs, peer, swap_sems, color, pos):
                copy.wait_send()


def grad_views(grads):
    g_qkv, g_proj, g_up, g_down = grads
    return [g.reshape(4, 4, 4, g.shape[0] // 64, g.shape[1]) for g in (g_up, g_down, g_qkv, g_proj)]


VMEM, DMA = pltpu.VMEM, pltpu.SemaphoreType.DMA
SWAP_SCRATCH = [VMEM((3, 4, 4, 4, 2, 8, 512), F32), VMEM((3, 4, 4, 4, 2, 8, 512), F32)]
PHASE_SCRATCH = [
    [VMEM((3, 2, 4, 4, 8, 512), F32), VMEM((3, 2, 2, 4, 4, 8, 512), F32)],
    [VMEM((3, 2, 4, 8, 512), F32), VMEM((3, 2, 2, 4, 8, 512), F32)],
    [VMEM((3, 2, 8, 512), F32), VMEM((3, 2, 2, 8, 512), F32)],
]
SWAP_SEMS = [DMA((3, 4, 3)), DMA((3, 4, 3)), DMA((3, 4, 3))]
PHASE_SEMS = lambda n: [DMA((3, n, 6)), DMA((3, n, 6))]
FINAL_SEMS = [DMA((3, 3)), DMA((3, 3))]


def reduce_grads(grads, which):
    args = grad_views(grads)
    outs = pl.pallas_call(
        reduce_kernel,
        in_specs=[pl.BlockSpec(memory_space=pl.ANY)] * 4,
        out_specs=[pl.BlockSpec(memory_space=VMEM)] * 4,
        out_shape=[jax.ShapeDtypeStruct(a.shape[3:], F32) for a in args],
        scratch_shapes=SWAP_SCRATCH + sum(PHASE_SCRATCH, []) + SWAP_SEMS + PHASE_SEMS(3) + FINAL_SEMS,
        compiler_params=pltpu.CompilerParams(collective_id=1 + which, has_side_effects=True, vmem_limit_bytes=30 << 20),
        name="reduce_grads",
    )(*args)
    return outs[2], outs[3], outs[0], outs[1]


def ffn_bwd_kernel(tile, carry, *refs):
    if not carry:
        refs = refs[1:]
    ge_ref, up_ref, ct_ref, n2_ref, mid_ref, at_ref, wd_ref, wu_ref, wp_ref = refs[:9]
    refs = refs[9:]
    step = pl.program_id(0)
    last = pl.num_programs(0) - 1
    at = lambda k, f: pl.when(step == k)(f)
    if carry:
        grads, refs = refs[:4], refs[4:]
        reduced = refs[5]
        acc_g, peer, near, final, load_sem, psend, precv, send_sem, recv_sem = refs[8:]
        red = Reducer(acc_g, ((near, final),), (send_sem, recv_sem))
        swap_sems = (psend, precv)
    gd_ref, gu_ref, gp_ref, cm_ref, ca_ref = refs[:5]
    acc, ctu = refs[6:8] if carry else refs[5:7]

    def every(what):
        for pos in range(4):
            for color in range(3):
                for copy in what(color, pos):
                    yield copy

    def begin():
        for copy in every(lambda color, pos: red.loads(grads, load_sem, color, pos)):
            copy.start()
        enter(red.me, red.partner)
        red.start_swaps(grads, peer, swap_sems, 0)

    def finish():
        red.fourth(0, reduced)
        red.drain(0)
        for copy in every(lambda color, pos: red.swaps(grads, peer, swap_sems, color, pos)):
            copy.wait_send()

    def swapped(*positions):
        for pos in positions:
            red.swapped(grads, peer, load_sem, swap_sems, pos)

    def carried_step():
        if carry:
            todo = {
                0: begin,
                1: lambda: swapped(0),
                2: lambda: swapped(1),
                3: lambda: swapped(2),
                4: lambda: (swapped(3), red.second(0))[0],
                6: lambda: red.third(0),
            }
            for k, f in todo.items():
                at(k, f)

    carried_step()
    chunks = range(0, ct_ref.shape[0], tile)
    for m in chunks:
        rows = slice(m, m + tile)
        cg = dot_nt(ct_ref[rows, :], wd_ref[...]).astype(BF).astype(F32)
        ctu[rows, :] = gelu_pull(up_ref[rows, :].astype(F32), cg).astype(BF)
    gd_ref[...] = dot_tn(ge_ref[...], ct_ref[...])
    gu_ref[...] = dot_tn(n2_ref[...], ctu[...])
    part = dot_nt(ctu[...], wu_ref[...])

    @pl.when(step == 0)
    def _():
        acc[...] = part

    @pl.when(step > 0)
    def _():
        acc[...] += part

    @pl.when(step == last)
    def _():
        pulled = rms_pull(mid_ref[...].astype(F32), acc[...].astype(BF).astype(F32))
        cm_ref[...] = (ct_ref[...].astype(F32) + pulled).astype(BF)
        ca_ref[...] = dot_nt(cm_ref[...], wp_ref[...]).astype(BF)
        gp_ref[...] = dot_tn(at_ref[...], cm_ref[...])

    if carry:
        at(last, finish)


def ffn_bwd(gelu, up, ct, first, normed2, mid, attn, w_down, w_up, w_proj, layer, tile, carried):
    tokens, d = mid.shape
    ff = gelu.shape[1]
    part = 256
    act = whole((tokens, d))
    cols = pl.BlockSpec((tokens, part), lambda i, *_: (0, i))
    ct_spec = act if carried is not None else pl.BlockSpec((tokens, d), lambda i, first: (first[0], 0), pipeline_mode=pl.Buffered(1))
    in_specs = [cols, cols, ct_spec, act, act, act,
                pl.BlockSpec((None, part, d), lambda i, *_: (layer, i, 0)), pl.BlockSpec((None, d, part), lambda i, *_: (layer, 0, i)), whole((d, d), layer)]
    out_specs = [pl.BlockSpec((part, d), lambda i, *_: (i, 0)), pl.BlockSpec((d, part), lambda i, *_: (0, i)), whole((d, d)), act, act]
    out_shape = [jax.ShapeDtypeStruct((ff, d), F32), jax.ShapeDtypeStruct((d, ff), F32), jax.ShapeDtypeStruct((d, d), F32),
                 jax.ShapeDtypeStruct((tokens, d), BF), jax.ShapeDtypeStruct((tokens, d), BF)]
    scratch = [VMEM((tokens, d), F32), VMEM((tokens, part), BF)]
    params = dict(vmem_limit_bytes=50 << 20)
    args = (gelu, up, ct, normed2, mid, attn, w_down, w_up, w_proj)
    carry = carried is not None
    if carry:
        args = args + tuple(grad_views(carried))
        first = None
        in_specs = in_specs + [pl.BlockSpec(memory_space=pl.ANY)] * 4
        out_specs = out_specs + [whole((3, 4, 4, 2, 8, 512))]
        out_shape = out_shape + [jax.ShapeDtypeStruct((3, 4, 4, 2, 8, 512), F32)]
        scratch = scratch + SWAP_SCRATCH + PHASE_SCRATCH[0] + SWAP_SEMS + PHASE_SEMS(1)
        params = dict(vmem_limit_bytes=62 << 20, collective_id=2, has_side_effects=True)
    return pl.pallas_call(
        functools.partial(ffn_bwd_kernel, tile, carry),
        grid_spec=pltpu.PrefetchScalarGridSpec(
            num_scalar_prefetch=0 if carry else 1, grid=(ff // part,), in_specs=in_specs, out_specs=out_specs, scratch_shapes=scratch),
        out_shape=out_shape,
        compiler_params=pltpu.CompilerParams(**params),
        name="ffn_bwd_carry" if carry else "ffn_bwd",
    )(*(args if carry else (first,) + args))


def attn_carry_kernel(scale, width, q_ref, k_ref, v_ref, do_ref, acc_hbm, dqkv_ref, *rest):
    results, (acc_ref, sup, sdown, sqkv, sproj, t1b, t2b, t1c, t2c, load_sem, send_sem, recv_sem, fsend_sem, frecv_sem) = rest[:4], rest[4:]
    steps = pl.num_programs(1)
    step = pl.program_id(0) * steps + pl.program_id(1)
    red = Reducer(acc_ref, (None, (t1b, t2b), (t1c, t2c)), (send_sem, recv_sem), start=1)
    outs, sems = (sup, sdown, sqkv, sproj), (fsend_sem, frecv_sem)

    def begin():
        load = pltpu.make_async_copy(acc_hbm, acc_ref, load_sem)
        load.start()
        enter(red.me, red.partner)
        load.wait()
        red.all_first(1)

    def turn():
        red.fourth(1)
        red.all_first(2)

    def close():
        red.fourth(2)
        give_finals(red, outs, sems)

    def third_second():
        red.third(1)

    todo = {0: begin, 2: lambda: red.second(1), 3: third_second, 4: turn, 5: lambda: red.second(2), 6: lambda: red.third(2), 7: close}
    for k, f in todo.items():
        pl.when(step == k)(f)
    attn_bwd_kernel(scale, width, q_ref, k_ref, v_ref, do_ref, dqkv_ref)

    @pl.when(step == pl.num_programs(0) * steps - 1)
    def _():
        end_finals(red, outs, sems)
        red.drain(1)
        red.drain(2)
        for result, out in zip(results, outs):
            result[...] = out[...]


def attn_bwd(qkv, do, seq, scale, carried):
    tokens, width = qkv.shape[0], qkv.shape[1] // 3
    steps = width // 256
    spec = lambda off: pl.BlockSpec((seq, 256), lambda b, j: (b, off + j))
    in_specs = [spec(0), spec(steps), spec(2 * steps), spec(0)]
    out_specs = [pl.BlockSpec((seq, 3 * width), lambda b, j: (b, 0))]
    out_shape = [jax.ShapeDtypeStruct((tokens, 3 * width), BF)]
    args, scratch, params, kernel = (qkv, qkv, qkv, do), [], {}, attn_bwd_kernel
    if carried is not None:
        args = args + (carried,)
        kernel = attn_carry_kernel
        in_specs = in_specs + [pl.BlockSpec(memory_space=pl.ANY)]
        shapes = ((8, 2048), (32, 512), (8, 1536), (8, 512))
        out_specs = out_specs + [whole(s) for s in shapes]
        out_shape = out_shape + [jax.ShapeDtypeStruct(s, F32) for s in shapes]
        scratch = [VMEM(s, F32) for s in (carried.shape,) + shapes] + PHASE_SCRATCH[1] + PHASE_SCRATCH[2] + [DMA] + PHASE_SEMS(2) + FINAL_SEMS
        params = dict(collective_id=3, has_side_effects=True, vmem_limit_bytes=50 << 20)
    return pl.pallas_call(
        functools.partial(kernel, scale, width),
        grid=(tokens // seq, steps), in_specs=in_specs, out_specs=out_specs, out_shape=out_shape, scratch_shapes=scratch,
        compiler_params=pltpu.CompilerParams(**params),
        name="attn_bwd" if carried is None else "attn_bwd_carry",
    )(*args)


def layer_forward(hidden, first, tokens, weights, layer, seq, scale):
    w_qkv, w_proj, w_up, w_down = weights
    normed, qkv = pre_attn(hidden, first, tokens, w_qkv, layer, seq)
    attn = attn_fwd(qkv, seq, scale)
    mid, normed2, up, gelu, out = post_attn(hidden, first, attn, w_proj, w_up, w_down, layer, seq)
    return out, (hidden, normed, qkv, attn, mid, normed2, up, gelu)


def layer_backward(saved, ct_out, first, weights, layer, seq, scale, carried):
    w_qkv, w_proj, w_up, w_down = weights
    hidden, normed, qkv, attn, mid, normed2, up, gelu = saved
    res = ffn_bwd(gelu, up, ct_out, first, normed2, mid, attn, w_down, w_up, w_proj, layer, seq, carried)
    g_down, g_up, g_proj, ct_mid, ct_attn = res[:5]
    res = attn_bwd(qkv, ct_attn, seq, scale, res[5] if carried is not None else None)
    ct_qkv = res[0]
    g_qkv = dot_tn(normed, ct_qkv)
    grads = (g_qkv, g_proj, g_up, g_down)
    if carried is not None:
        return grads, (res[3], res[4], res[1], res[2])
    ct_norm = dot_nt(ct_qkv, w_qkv[layer]).astype(BF)
    ct_hidden = (ct_mid.astype(F32) + rms_pull(hidden.astype(F32), ct_norm.astype(F32))).astype(BF)
    return grads, ct_hidden


def solution(mesh):
    stages = mesh.shape['pp']
    grid = Mesh(mesh.devices.reshape(2, 4, 4, 4), ("pp", "z", "y", "x"))
    dp = ("z", "y", "x")
    swap = [(0, 1), (1, 0)]

    def device_step(act_in, loss_seed, w_qkv, w_proj, w_up, w_down):
        micro, _, seq, d = act_in.shape
        mine = micro // 2
        pp = lax.axis_index('pp')
        heads3, hd = w_qkv.shape[2:]
        scale = hd ** -0.5

        full = gather_weights(*(w.reshape(w.shape[1], -1) for w in (w_qkv, w_proj, w_up, w_down)))
        tokens = mine * seq
        act, seed = act_in.reshape(micro * seq, d), loss_seed.reshape(micro * seq, d)
        pp_vec, none = jnp.full((1,), pp, jnp.int32), jnp.zeros((1,), jnp.int32)
        h1, saved0 = layer_forward(act, pp_vec * mine, tokens, full, 0, seq, scale)
        h2, saved1 = layer_forward(h1, none, tokens, full, 1, seq, scale)

        out4 = h2.reshape(mine, 1, seq, d)
        half = seq // 2
        keep = lax.dynamic_slice_in_dim(out4, pp * half, half, 2)
        give = lax.dynamic_slice_in_dim(out4, (1 - pp) * half, half, 2)
        got = lax.ppermute(give, 'pp', swap)
        act_out = jnp.concatenate([jnp.where(pp == 0, keep, got), jnp.where(pp == 0, got, keep)], axis=0)

        grads1, ct1 = layer_backward(saved1, seed, pp_vec, full, 1, seq, scale, None)
        grads0, red1 = layer_backward(saved0, ct1, None, full, 0, seq, scale, grads1)
        red0 = reduce_grads(grads0, 0)
        outs = [jnp.where(pp == 0, a, b) for a, b in zip(red0, red1)]
        return tuple(o.reshape(w.shape) for o, w in zip(outs, (w_qkv, w_proj, w_up, w_down))) + (act_out,)

    weight_spec = P('pp', dp)
    act_spec = P(None, dp)
    return jax.shard_map(device_step, mesh=grid, in_specs=(act_spec, act_spec) + (weight_spec,) * 4, out_specs=(weight_spec,) * 4 + (P(None, dp, 'pp'),), check_vma=False)
```

```python
import functools

import jax
import jax.numpy as jnp
from jax import lax
from jax.experimental import pallas as pl
from jax.experimental.pallas import tpu as pltpu
from jax.sharding import Mesh
from jax.sharding import PartitionSpec as P

NORM_EPS = 1e-6
BF = jnp.bfloat16
F32 = jnp.float32


def rms_norm(hidden):
    return hidden * lax.rsqrt(jnp.mean(hidden * hidden, axis=-1, keepdims=True) + NORM_EPS)


def dot(a, b):
    return lax.dot_general(a, b, (((1,), (0,)), ((), ())), preferred_element_type=F32)


def dot_nt(a, b):
    return lax.dot_general(a, b, (((1,), (1,)), ((), ())), preferred_element_type=F32)


def dot_tn(a, b):
    return lax.dot_general(a, b, (((0,), (0,)), ((), ())), preferred_element_type=F32)


LOG2E = 1.4426950408889634
GELU_A = 0.7978845608028654
GELU_B = GELU_A * 0.044715


def split_heads(refs, count):
    low = lax.broadcasted_iota(jnp.int32, (refs[0].shape[0], 128), 1) < 64
    zero = jnp.zeros((refs[0].shape[0], 128), BF)
    heads = []
    for h in range(count):
        keep = low if h % 2 == 0 else jnp.logical_not(low)
        lanes = slice((h // 2) * 128, (h // 2) * 128 + 128)
        heads.append([(r[:, lanes], jnp.where(keep, r[:, lanes], zero)) for r in refs])
    return heads


def causal_mask(n):
    return lax.broadcasted_iota(jnp.int32, (n, n), 0) >= lax.broadcasted_iota(jnp.int32, (n, n), 1)


def softmax_rows(s, keep, scale):
    s = jnp.where(keep, s, -1e30)
    e = jnp.exp2((s - jnp.max(s, axis=-1, keepdims=True)) * (scale * LOG2E))
    return e * (1.0 / jnp.sum(e, axis=-1, keepdims=True))


def row_blocks(seq, parts):
    return parts if seq == parts[-1][1] else ((0, seq),)


def attn_fwd_kernel(scale, q_ref, k_ref, v_ref, o_ref):
    seq, lanes = q_ref.shape
    count = lanes // 64
    blocks = row_blocks(seq, ((0, 128), (128, 256), (256, 384)))
    keep = causal_mask(seq)
    heads = split_heads((q_ref, k_ref, v_ref), count)
    scores = [[dot_nt(q[0][a:b], k[1][:b]) for a, b in blocks] for q, k, v in heads]
    probs = [[softmax_rows(s, keep[a:b, :b], scale).astype(BF) for (a, b), s in zip(blocks, row)] for row in scores]
    for h in range(0, count, 2):
        for n, (a, b) in enumerate(blocks):
            pair = dot(probs[h][n], heads[h][2][1][:b]) + dot(probs[h + 1][n], heads[h + 1][2][1][:b])
            o_ref[a:b, (h // 2) * 128:(h // 2) * 128 + 128] = pair.astype(BF)


def attn_bwd_kernel(scale, width, q_ref, k_ref, v_ref, do_ref, dqkv_ref):
    seq, lanes = q_ref.shape
    count = lanes // 64
    blocks = row_blocks(seq, ((0, 256), (256, 384)))
    keep = causal_mask(seq)
    base = pl.program_id(1) * lanes
    heads = split_heads((q_ref, k_ref, v_ref, do_ref), count)
    firsts = [[(dot_nt(q[0][a:b], k[1][:b]), dot_nt(do[0][a:b], v[1][:b])) for a, b in blocks] for q, k, v, do in heads]
    work = []
    for row in firsts:
        done = []
        for (a, b), (s, dp) in zip(blocks, row):
            p = softmax_rows(s, keep[a:b, :b], scale)
            dp = dp.astype(BF).astype(F32)
            delta = jnp.sum(dp * p, axis=-1, keepdims=True)
            done.append((p.astype(BF), (p * (dp - delta) * scale).astype(BF)))
        work.append(done)
    total = lambda terms: functools.reduce(lambda x, y: x + y, terms)
    for j in range(count // 2):
        pair = (2 * j, 2 * j + 1)
        cols = [pl.ds(pl.multiple_of(base + j * 128 + i * width, 128), 128) for i in range(3)]
        for n, (a, b) in enumerate(blocks):
            dqkv_ref[a:b, cols[0]] = total([dot(work[h][n][1], heads[h][1][1][:b]) for h in pair]).astype(BF)
        for i, (_, hi) in enumerate(blocks):
            lo = blocks[i - 1][1] if i else 0
            later = [(n, a, b, h) for n, (a, b) in enumerate(blocks) if n >= i for h in pair]
            dqkv_ref[lo:hi, cols[1]] = total([dot_tn(work[h][n][1][:, lo:hi], heads[h][0][1][a:b]) for n, a, b, h in later]).astype(BF)
            dqkv_ref[lo:hi, cols[2]] = total([dot_tn(work[h][n][0][:, lo:hi], heads[h][3][1][a:b]) for n, a, b, h in later]).astype(BF)


def attn_fwd(qkv, seq, scale):
    tokens, width = qkv.shape[0], qkv.shape[1] // 3
    spec = lambda off: pl.BlockSpec((seq, width), lambda b: (b, off))
    return pl.pallas_call(
        functools.partial(attn_fwd_kernel, scale),
        grid=(tokens // seq,),
        in_specs=[spec(0), spec(1), spec(2)],
        out_specs=spec(0),
        out_shape=jax.ShapeDtypeStruct((tokens, width), BF),
        name="attn_fwd",
    )(qkv, qkv, qkv)


def pre_kernel(_, h_ref, w_ref, n_ref, qkv_ref):
    normed = rms_norm(h_ref[...].astype(F32)).astype(BF)
    n_ref[...] = normed
    qkv_ref[...] = dot(normed, w_ref[...]).astype(BF)


def whole(shape, layer=None):
    block = shape if layer is None else (None,) + shape
    index = (0,) * len(shape) if layer is None else (layer,) + (0,) * len(shape)
    return pl.BlockSpec(block, lambda *_: index, pipeline_mode=pl.Buffered(1))


def rows_at(tile, n, shifted=False):
    return pl.BlockSpec((tile, n), lambda i, first: (i + first[0] if shifted else i, 0))


def pre_attn(hidden, first, tokens, w_qkv, layer, tile):
    d = hidden.shape[1]
    cols = w_qkv.shape[2]
    return pl.pallas_call(
        pre_kernel,
        grid_spec=pltpu.PrefetchScalarGridSpec(
            num_scalar_prefetch=1, grid=(tokens // tile,),
            in_specs=[rows_at(tile, d, True), whole((d, cols), layer)],
            out_specs=[rows_at(tile, d), rows_at(tile, cols)]),
        out_shape=[jax.ShapeDtypeStruct((tokens, d), BF), jax.ShapeDtypeStruct((tokens, cols), BF)],
        name="pre_attn",
    )(first, hidden, w_qkv)


def post_kernel(_, h_ref, a_ref, wp_ref, wu_ref, wd_ref, mid_ref, n2_ref, up_ref, ge_ref, out_ref):
    mid = (h_ref[...].astype(F32) + dot(a_ref[...], wp_ref[...])).astype(BF)
    mid_ref[...] = mid
    mid_f32 = mid.astype(F32)
    n2 = rms_norm(mid_f32).astype(BF)
    n2_ref[...] = n2
    ff = wu_ref.shape[1]
    for c in range(0, ff, 512):
        up = dot(n2, wu_ref[:, c:c + 512]).astype(BF)
        up_ref[:, c:c + 512] = up
        u = up.astype(F32)
        t = jnp.tanh(u * (GELU_A + GELU_B * (u * u)))
        ge_ref[:, c:c + 512] = (u * (0.5 * t + 0.5)).astype(BF)
    out_ref[...] = (mid_f32 + dot(ge_ref[...], wd_ref[...])).astype(BF)


def post_attn(hidden, first, attn, w_proj, w_up, w_down, layer, tile):
    tokens, d = attn.shape
    ff = w_up.shape[2]
    sizes = (d, d, ff, ff, d)
    return pl.pallas_call(
        post_kernel,
        grid_spec=pltpu.PrefetchScalarGridSpec(
            num_scalar_prefetch=1, grid=(tokens // tile,),
            in_specs=[rows_at(tile, d, True), rows_at(tile, d), whole((d, d), layer), whole((d, ff), layer), whole((ff, d), layer)],
            out_specs=[rows_at(tile, n) for n in sizes]),
        out_shape=[jax.ShapeDtypeStruct((tokens, n), BF) for n in sizes],
        name="post_attn",
    )(first, hidden, attn, w_proj, w_up, w_down)


def gelu_pull(u, g):
    u2 = u * u
    s = 0.5 * jnp.tanh(u * (GELU_A + GELU_B * u2)) + 0.5
    return g * (s + (s - s * s) * (u * (2 * GELU_A + (6 * GELU_B) * u2)))


def rms_pull(m, g):
    r = lax.rsqrt(jnp.mean(m * m, axis=-1, keepdims=True) + NORM_EPS)
    return g * r - m * (r * r * r * jnp.mean(g * m, axis=-1, keepdims=True))


MESH = pl.DeviceIdType.MESH
AXES = ("z", "y", "x")
GATHER_ORDER = ((2, 1, 0), (0, 2, 1), (1, 0, 2))
REDUCE_ORDER = ((0, 1, 2), (1, 2, 0), (2, 0, 1))


def step_coord(pos, by):
    return lax.rem(pos + by, 4)


def neighbour(me, axis, by):
    return {AXES[axis]: step_coord(me[axis], by)}


def enter(me, partner):
    barrier = pltpu.get_barrier_semaphore()
    for axis in range(3):
        for by in (1, 3):
            pl.semaphore_signal(barrier, inc=1, device_id=neighbour(me, axis, by), device_id_type=MESH)
    pl.semaphore_signal(barrier, inc=1, device_id={"pp": partner}, device_id_type=MESH)
    pl.semaphore_wait(barrier, 7)


def remote(src, dst, send, recv, where):
    copy = pltpu.make_async_remote_copy(src_ref=src, dst_ref=dst, send_sem=send, recv_sem=recv, device_id=where, device_id_type=MESH)
    copy.start()
    return copy


def gather_kernel(up_ref, down_ref, qkv_ref, proj_ref, *rest):
    results, bufs, (local_sem, send_sem, recv_sem, psend_sem, precv_sem, out_sem) = rest[:4], rest[4:8], rest[8:]
    pp = lax.axis_index("pp")
    partner = 1 - pp
    me = tuple(lax.axis_index(a) for a in AXES)
    sources = (up_ref, down_ref, qkv_ref, proj_ref)
    groups = (0, 1, 2, 2)

    def region(base, n, phase, by, half, layer):
        order = GATHER_ORDER[groups[n]]
        idx = [None, None, None]
        for later, axis in enumerate(order):
            idx[axis] = slice(None) if later < phase else step_coord(me[axis], by if later == phase else 0)
        rows, cols = base[n].shape[-2:]
        tail = (slice(None), slice(None))
        if half is not None and rows > 8:
            tail = (pl.ds(half * (rows // 2), rows // 2), slice(None))
        elif half is not None:
            tail = (slice(None), pl.ds(half * (cols // 2), cols // 2))
        return base[n].at[(layer,) + tuple(idx) + tail]

    own = [pltpu.make_async_copy(src, bufs[n].at[(pp,) + me], local_sem.at[n]) for n, src in enumerate(sources)]
    for copy in own:
        copy.start()
    enter(me, partner)
    for copy in own:
        copy.wait()

    sends, partners, locals_ = [], [], []

    def put_out(n, slot, by, half, layer, side):
        copy = pltpu.make_async_copy(region(bufs, n, 2, by, half, layer), region(results, n, 2, by, half, layer), out_sem.at[n, slot, side])
        copy.start()
        locals_.append(copy)

    def ready(n, slot, by, half):
        ref = region(bufs, n, 2, by, half, pp)
        copy = remote(ref, ref, psend_sem.at[n, slot], precv_sem.at[n, slot], {"pp": partner})
        partners.append((copy, n, slot, by, half))
        put_out(n, slot, by, half, pp, 0)

    def send(n, phase, slot, by, half, to):
        axis = GATHER_ORDER[groups[n]][phase]
        ref = region(bufs, n, phase, by, half, pp)
        sends.append(remote(ref, ref, send_sem.at[n, phase, slot], recv_sem.at[n, phase, slot], neighbour(me, axis, to)))

    def arrived(n, phase, slot, by, half):
        ref = region(bufs, n, phase, by, half, pp)
        pltpu.make_async_copy(ref, ref, recv_sem.at[n, phase, slot]).wait()
        if phase == 2:
            ready(n, slot + 1, by, half)

    for phase in range(3):
        for n in range(4):
            send(n, phase, 0, 0, 0, 1)
            send(n, phase, 1, 0, 1, 3)
        for n in range(4):
            send(n, phase, 2, 0, 1, 1)
            send(n, phase, 3, 0, 0, 3)
            if phase == 2:
                ready(n, 0, 0, None)
        for n in range(4):
            arrived(n, phase, 0, 3, 0)
            send(n, phase, 4, 3, 0, 1)
            arrived(n, phase, 1, 1, 1)
            send(n, phase, 5, 1, 1, 3)
        for n in range(4):
            arrived(n, phase, 2, 3, 1)
            arrived(n, phase, 3, 1, 0)
        for n in range(4):
            arrived(n, phase, 4, 2, 0)
            arrived(n, phase, 5, 2, 1)
    for copy, n, slot, by, half in partners:
        copy.wait_recv()
        put_out(n, slot, by, half, partner, 1)
    for copy in sends:
        copy.wait_send()
    for copy, *_ in partners:
        copy.wait_send()
    for copy in locals_:
        copy.wait()


def gather_weights(w_qkv, w_proj, w_up, w_down):
    vmem = pl.BlockSpec(memory_space=pltpu.VMEM)
    shape = lambda w: (2, 4, 4, 4) + w.shape
    dma = pltpu.SemaphoreType.DMA
    args = (w_up, w_down, w_qkv, w_proj)
    outs = pl.pallas_call(
        gather_kernel,
        in_specs=[vmem] * 4,
        out_specs=[pl.BlockSpec(memory_space=pltpu.HBM)] * 4,
        out_shape=[jax.ShapeDtypeStruct(shape(w), BF) for w in args],
        scratch_shapes=[pltpu.VMEM(shape(w), BF) for w in args] + [dma((4,)), dma((4, 3, 6)), dma((4, 3, 6)), dma((4, 7)), dma((4, 7)), dma((4, 7, 2))],
        compiler_params=pltpu.CompilerParams(collective_id=0, has_side_effects=True, vmem_limit_bytes=62 << 20),
        name="gather_weights",
    )(*args)
    flat = [o.reshape(2, -1, o.shape[-1]) for o in outs]
    return flat[2], flat[3], flat[0], flat[1]


REDUCE_OFFSETS = (2, 1, 3, 0)


def reduce_pieces(refs, color, core):
    up_ref, down_ref, qkv_ref, proj_ref = refs
    if color == 0:
        return [(up_ref, pl.ds(0, 8), pl.ds(pl.multiple_of(core * 1024 + h * 512, 128), 512), h, pl.ds(0, 512)) for h in range(2)]
    if color == 1:
        return [(down_ref, pl.ds(pl.multiple_of(core * 16 + h * 8, 8), 8), pl.ds(0, 512), h, pl.ds(0, 512)) for h in range(2)]
    return [
        (qkv_ref, pl.ds(0, 8), pl.ds(pl.multiple_of(core * 768, 128), 512), 0, pl.ds(0, 512)),
        (qkv_ref, pl.ds(0, 8), pl.ds(pl.multiple_of(core * 768 + 512, 128), 256), 1, pl.ds(0, 256)),
        (proj_ref, pl.ds(0, 8), pl.ds(pl.multiple_of(core * 256, 128), 256), 1, pl.ds(256, 256)),
    ]


def add_block(out, dst, src):
    if len(dst.shape) < 4:
        out[...] = dst[...] + src[...]
        return

    def body(i, _):
        out[i] = dst[i] + src[i]
        return 0

    lax.fori_loop(0, dst.shape[0], body, 0)


class Reducer:
    def __init__(self, acc, slots, sems, start=0):
        self.pp = lax.axis_index("pp")
        self.partner = 1 - self.pp
        self.me = tuple(lax.axis_index(a) for a in AXES)
        self.acc, self.slots, self.start = acc, slots, start
        self.send_sem, self.recv_sem = sems

    def lead(self, color, phase, where):
        order = REDUCE_ORDER[color]
        idx = [None, None, None]
        for later, axis in enumerate(order):
            idx[axis] = self.me[axis] if later < phase else (where if later == phase else slice(None))
        return tuple(v for axis, v in enumerate(idx) if order.index(axis) >= self.start)

    def place(self, color, phase, by):
        return step_coord(self.me[REDUCE_ORDER[color][phase]], by)

    def loads(self, refs, sem, color, pos):
        where = self.lead(color, 0, self.place(color, 0, REDUCE_OFFSETS[pos]))
        return [
            pltpu.make_async_copy(ref.at[where + (rows, cols)], self.acc.at[(color,) + where + (h, slice(None), into)], sem.at[color, pos, n])
            for n, (ref, rows, cols, h, into) in enumerate(reduce_pieces(refs, color, self.pp))
        ]

    def swaps(self, refs, peer, sems, color, pos):
        where = self.lead(color, 0, self.place(color, 0, REDUCE_OFFSETS[pos]))
        return [
            pltpu.make_async_remote_copy(
                src_ref=ref.at[where + (rows, cols)], dst_ref=peer.at[(color,) + where + (h, slice(None), into)],
                send_sem=sems[0].at[color, pos, n], recv_sem=sems[1].at[color, pos, n], device_id={"pp": self.partner}, device_id_type=MESH)
            for n, (ref, rows, cols, h, into) in enumerate(reduce_pieces(refs, color, self.partner))
        ]

    def part(self, color, phase, by, half):
        return self.acc.at[(color,) + self.lead(color, phase, self.place(color, phase, by)) + (half,)]

    def near(self, color, phase, side):
        return self.slots[phase][0].at[color, side]

    def final(self, color, phase, side, half):
        return self.slots[phase][1].at[color, side, half]

    def copy(self, color, phase, n):
        part, near, final = self.part, self.near, self.final
        plan = (
            (part(color, phase, 2, 0), near(color, phase, 0), 1),
            (part(color, phase, 2, 1), near(color, phase, 1), 3),
            (part(color, phase, 1, 1), final(color, phase, 0, 1), 1),
            (part(color, phase, 3, 0), final(color, phase, 1, 0), 3),
            (part(color, phase, 1, 0), final(color, phase, 0, 0), 1),
            (part(color, phase, 3, 1), final(color, phase, 1, 1), 3),
        )
        k = phase - self.start
        src, dst, by = plan[n]
        return pltpu.make_async_remote_copy(
            src_ref=src, dst_ref=dst, send_sem=self.send_sem.at[color, k, n], recv_sem=self.recv_sem.at[color, k, n],
            device_id=neighbour(self.me, REDUCE_ORDER[color][phase], by), device_id_type=MESH)

    def first_sends(self, color, phase, by):
        for n in {2: (0, 1), 1: (2,), 3: (3,), 0: ()}[by]:
            self.copy(color, phase, n).start()

    def start_swaps(self, refs, peer, swap_sems, pos):
        if pos < 4:
            for color in range(3):
                for copy in self.swaps(refs, peer, swap_sems, color, pos):
                    copy.start()

    def swapped(self, refs, peer, load_sem, swap_sems, pos):
        by = REDUCE_OFFSETS[pos]
        for color in range(3):
            for copy in self.loads(refs, load_sem, color, pos):
                copy.wait()
            for copy in self.swaps(refs, peer, swap_sems, color, pos):
                copy.wait_recv()
        self.start_swaps(refs, peer, swap_sems, pos + 1)
        for color in range(3):
            block = self.acc.at[(color,) + self.lead(color, 0, self.place(color, 0, by))]
            add_block(block, block, peer.at[(color,) + self.lead(color, 0, self.place(color, 0, by))])
            self.first_sends(color, 0, by)

    def all_first(self, phase):
        for by in (2, 1, 3):
            for color in range(3):
                self.first_sends(color, phase, by)

    def second(self, phase):
        for color in range(3):
            for n, by, half in ((0, 1, 0), (1, 3, 1)):
                self.copy(color, phase, n).wait_recv()
                dst = self.part(color, phase, by, half)
                add_block(dst, dst, self.near(color, phase, n))
                self.copy(color, phase, n + 4).start()

    def third(self, phase):
        for color in range(3):
            for n, side, half in ((2, 0, 1), (3, 1, 0)):
                self.copy(color, phase, n).wait_recv()
                dst = self.part(color, phase, 0, half)
                add_block(dst, dst, self.final(color, phase, side, half))

    def fourth(self, phase, out=None):
        for color in range(3):
            for n, side, half in ((4, 0, 0), (5, 1, 1)):
                self.copy(color, phase, n).wait_recv()
                dst = self.part(color, phase, 0, half)
                add_block(dst if out is None else out.at[color, :, :, half], dst, self.final(color, phase, side, half))

    def drain(self, phase):
        for color in range(3):
            for n in range(6):
                self.copy(color, phase, n).wait_send()

    def finals(self, outs, sems):
        copies = []
        for color in range(3):
            for n, (out, rows, cols, h, into) in enumerate(reduce_pieces(outs, color, self.pp)):
                where = self.lead(color, 3, None)
                copies.append((out.at[rows, cols], self.acc.at[(color,) + where + (h, slice(None), into)], pltpu.make_async_remote_copy(
                    src_ref=self.acc.at[(color,) + where + (h, slice(None), into)], dst_ref=out.at[rows, cols],
                    send_sem=sems[0].at[color, n], recv_sem=sems[1].at[color, n], device_id={"pp": self.partner}, device_id_type=MESH)))
        return copies


def give_finals(red, outs, sems):
    for dst, src, copy in red.finals(outs, sems):
        copy.start()
        dst[...] = src[...]


def end_finals(red, outs, sems):
    for _, _, copy in red.finals(outs, sems):
        copy.wait_send()
        copy.wait_recv()


def reduce_kernel(up_ref, down_ref, qkv_ref, proj_ref, oup, odown, oqkv, oproj,
                  acc, peer, t1a, t2a, t1b, t2b, t1c, t2c,
                  load_sem, psend_sem, precv_sem, send_sem, recv_sem, fsend_sem, frecv_sem):
    refs, outs = (up_ref, down_ref, qkv_ref, proj_ref), (oup, odown, oqkv, oproj)
    red = Reducer(acc, ((t1a, t2a), (t1b, t2b), (t1c, t2c)), (send_sem, recv_sem))
    swap_sems, final_sems = (psend_sem, precv_sem), (fsend_sem, frecv_sem)
    for pos in range(4):
        for color in range(3):
            for copy in red.loads(refs, load_sem, color, pos):
                copy.start()
    enter(red.me, red.partner)
    red.start_swaps(refs, peer, swap_sems, 0)
    for pos in range(4):
        red.swapped(refs, peer, load_sem, swap_sems, pos)
    for phase in range(3):
        if phase:
            red.all_first(phase)
        red.second(phase)
        red.third(phase)
        red.fourth(phase)
    give_finals(red, outs, final_sems)
    end_finals(red, outs, final_sems)
    for phase in range(3):
        red.drain(phase)
    for pos in range(4):
        for color in range(3):
            for copy in red.swaps(refs, peer, swap_sems, color, pos):
                copy.wait_send()


def grad_views(grads):
    g_qkv, g_proj, g_up, g_down = grads
    return [g.reshape(4, 4, 4, g.shape[0] // 64, g.shape[1]) for g in (g_up, g_down, g_qkv, g_proj)]


VMEM, DMA = pltpu.VMEM, pltpu.SemaphoreType.DMA
SWAP_SCRATCH = [VMEM((3, 4, 4, 4, 2, 8, 512), F32), VMEM((3, 4, 4, 4, 2, 8, 512), F32)]
PHASE_SCRATCH = [
    [VMEM((3, 2, 4, 4, 8, 512), F32), VMEM((3, 2, 2, 4, 4, 8, 512), F32)],
    [VMEM((3, 2, 4, 8, 512), F32), VMEM((3, 2, 2, 4, 8, 512), F32)],
    [VMEM((3, 2, 8, 512), F32), VMEM((3, 2, 2, 8, 512), F32)],
]
SWAP_SEMS = [DMA((3, 4, 3)), DMA((3, 4, 3)), DMA((3, 4, 3))]
PHASE_SEMS = lambda n: [DMA((3, n, 6)), DMA((3, n, 6))]
FINAL_SEMS = [DMA((3, 3)), DMA((3, 3))]


def reduce_grads(grads, which):
    args = grad_views(grads)
    outs = pl.pallas_call(
        reduce_kernel,
        in_specs=[pl.BlockSpec(memory_space=pl.ANY)] * 4,
        out_specs=[pl.BlockSpec(memory_space=VMEM)] * 4,
        out_shape=[jax.ShapeDtypeStruct(a.shape[3:], F32) for a in args],
        scratch_shapes=SWAP_SCRATCH + sum(PHASE_SCRATCH, []) + SWAP_SEMS + PHASE_SEMS(3) + FINAL_SEMS,
        compiler_params=pltpu.CompilerParams(collective_id=1 + which, has_side_effects=True, vmem_limit_bytes=30 << 20),
        name="reduce_grads",
    )(*args)
    return outs[2], outs[3], outs[0], outs[1]


def ffn_bwd_kernel(tile, carry, *refs):
    if not carry:
        refs = refs[1:]
    ge_ref, up_ref, ct_ref, n2_ref, mid_ref, at_ref, wd_ref, wu_ref, wp_ref = refs[:9]
    refs = refs[9:]
    step = pl.program_id(0)
    last = pl.num_programs(0) - 1
    at = lambda k, f: pl.when(step == k)(f)
    if carry:
        grads, refs = refs[:4], refs[4:]
        reduced = refs[5]
        acc_g, peer, near, final, load_sem, psend, precv, send_sem, recv_sem = refs[8:]
        red = Reducer(acc_g, ((near, final),), (send_sem, recv_sem))
        swap_sems = (psend, precv)
    gd_ref, gu_ref, gp_ref, cm_ref, ca_ref = refs[:5]
    acc, ctu = refs[6:8] if carry else refs[5:7]

    def every(what):
        for pos in range(4):
            for color in range(3):
                for copy in what(color, pos):
                    yield copy

    def begin():
        for copy in every(lambda color, pos: red.loads(grads, load_sem, color, pos)):
            copy.start()
        enter(red.me, red.partner)
        red.start_swaps(grads, peer, swap_sems, 0)

    def finish():
        red.fourth(0, reduced)
        red.drain(0)
        for copy in every(lambda color, pos: red.swaps(grads, peer, swap_sems, color, pos)):
            copy.wait_send()

    def swapped(*positions):
        for pos in positions:
            red.swapped(grads, peer, load_sem, swap_sems, pos)

    def carried_step():
        if carry:
            todo = {
                0: begin,
                1: lambda: swapped(0),
                2: lambda: swapped(1),
                3: lambda: swapped(2),
                4: lambda: (swapped(3), red.second(0))[0],
                6: lambda: red.third(0),
            }
            for k, f in todo.items():
                at(k, f)

    carried_step()
    chunks = range(0, ct_ref.shape[0], tile)
    for m in chunks:
        rows = slice(m, m + tile)
        cg = dot_nt(ct_ref[rows, :], wd_ref[...]).astype(BF).astype(F32)
        ctu[rows, :] = gelu_pull(up_ref[rows, :].astype(F32), cg).astype(BF)
    gd_ref[...] = dot_tn(ge_ref[...], ct_ref[...])
    gu_ref[...] = dot_tn(n2_ref[...], ctu[...])
    acc[...] = jnp.where(step == 0, 0.0, acc[...]) + dot_nt(ctu[...], wu_ref[...])

    @pl.when(step == last)
    def _():
        pulled = rms_pull(mid_ref[...].astype(F32), acc[...].astype(BF).astype(F32))
        cm_ref[...] = (ct_ref[...].astype(F32) + pulled).astype(BF)
        ca_ref[...] = dot_nt(cm_ref[...], wp_ref[...]).astype(BF)
        gp_ref[...] = dot_tn(at_ref[...], cm_ref[...])

    if carry:
        at(last, finish)


def ffn_bwd(gelu, up, ct, first, normed2, mid, attn, w_down, w_up, w_proj, layer, tile, carried):
    tokens, d = mid.shape
    ff = gelu.shape[1]
    part = 256
    act = whole((tokens, d))
    cols = pl.BlockSpec((tokens, part), lambda i, *_: (0, i))
    ct_spec = act if carried is not None else pl.BlockSpec((tokens, d), lambda i, first: (first[0], 0), pipeline_mode=pl.Buffered(1))
    in_specs = [cols, cols, ct_spec, act, act, act,
                pl.BlockSpec((None, part, d), lambda i, *_: (layer, i, 0)), pl.BlockSpec((None, d, part), lambda i, *_: (layer, 0, i)), whole((d, d), layer)]
    out_specs = [pl.BlockSpec((part, d), lambda i, *_: (i, 0)), pl.BlockSpec((d, part), lambda i, *_: (0, i)), whole((d, d)), act, act]
    out_shape = [jax.ShapeDtypeStruct((ff, d), F32), jax.ShapeDtypeStruct((d, ff), F32), jax.ShapeDtypeStruct((d, d), F32),
                 jax.ShapeDtypeStruct((tokens, d), BF), jax.ShapeDtypeStruct((tokens, d), BF)]
    scratch = [VMEM((tokens, d), F32), VMEM((tokens, part), BF)]
    params = dict(vmem_limit_bytes=50 << 20)
    args = (gelu, up, ct, normed2, mid, attn, w_down, w_up, w_proj)
    carry = carried is not None
    if carry:
        args = args + tuple(grad_views(carried))
        first = None
        in_specs = in_specs + [pl.BlockSpec(memory_space=pl.ANY)] * 4
        out_specs = out_specs + [whole((3, 4, 4, 2, 8, 512))]
        out_shape = out_shape + [jax.ShapeDtypeStruct((3, 4, 4, 2, 8, 512), F32)]
        scratch = scratch + SWAP_SCRATCH + PHASE_SCRATCH[0] + SWAP_SEMS + PHASE_SEMS(1)
        params = dict(vmem_limit_bytes=62 << 20, collective_id=2, has_side_effects=True)
    return pl.pallas_call(
        functools.partial(ffn_bwd_kernel, tile, carry),
        grid_spec=pltpu.PrefetchScalarGridSpec(
            num_scalar_prefetch=0 if carry else 1, grid=(ff // part,), in_specs=in_specs, out_specs=out_specs, scratch_shapes=scratch),
        out_shape=out_shape,
        compiler_params=pltpu.CompilerParams(**params),
        name="ffn_bwd_carry" if carry else "ffn_bwd",
    )(*(args if carry else (first,) + args))


def attn_carry_kernel(scale, width, q_ref, k_ref, v_ref, do_ref, acc_hbm, h2_hbm, dqkv_ref, *rest):
    results, act_hbm = rest[:4], rest[4]
    acc_ref, sup, sdown, sqkv, sproj, t1b, t2b, t1c, t2c, load_sem, send_sem, recv_sem, fsend_sem, frecv_sem, act_sem = rest[5:]
    steps = pl.num_programs(1)
    step = pl.program_id(0) * steps + pl.program_id(1)
    red = Reducer(acc_ref, (None, (t1b, t2b), (t1c, t2c)), (send_sem, recv_sem), start=1)
    outs, sems = (sup, sdown, sqkv, sproj), (fsend_sem, frecv_sem)

    def act_copies():
        where = act_hbm.at[pl.ds(red.pp * h2_hbm.shape[0], h2_hbm.shape[0])]
        keep = pltpu.make_async_copy(h2_hbm.at[:, red.pp], where, act_sem.at[0])
        give = pltpu.make_async_remote_copy(
            src_ref=h2_hbm.at[:, red.partner], dst_ref=where, send_sem=act_sem.at[1], recv_sem=act_sem.at[2],
            device_id={"pp": red.partner}, device_id_type=MESH)
        come = pltpu.make_async_copy(h2_hbm.at[:, red.pp], act_hbm.at[pl.ds(red.partner * h2_hbm.shape[0], h2_hbm.shape[0])], act_sem.at[2])
        return keep, give, come

    def begin():
        load = pltpu.make_async_copy(acc_hbm, acc_ref, load_sem)
        load.start()
        enter(red.me, red.partner)
        load.wait()
        red.all_first(1)
        keep, give, _ = act_copies()
        keep.start()
        give.start()

    def turn():
        red.fourth(1)
        red.all_first(2)

    def close():
        red.fourth(2)
        give_finals(red, outs, sems)

    def third_second():
        red.third(1)

    todo = {0: begin, 2: lambda: red.second(1), 3: third_second, 4: turn, 5: lambda: red.second(2), 6: lambda: red.third(2), 7: close}
    for k, f in todo.items():
        pl.when(step == k)(f)
    attn_bwd_kernel(scale, width, q_ref, k_ref, v_ref, do_ref, dqkv_ref)

    @pl.when(step == pl.num_programs(0) * steps - 1)
    def _():
        end_finals(red, outs, sems)
        red.drain(1)
        red.drain(2)
        keep, give, come = act_copies()
        keep.wait()
        give.wait_send()
        come.wait()
        for result, out in zip(results, outs):
            result[...] = out[...]


def attn_bwd(qkv, do, seq, scale, carried, h2):
    tokens, width = qkv.shape[0], qkv.shape[1] // 3
    steps = width // 256
    spec = lambda off: pl.BlockSpec((seq, 256), lambda b, j: (b, off + j))
    in_specs = [spec(0), spec(steps), spec(2 * steps), spec(0)]
    out_specs = [pl.BlockSpec((seq, 3 * width), lambda b, j: (b, 0))]
    out_shape = [jax.ShapeDtypeStruct((tokens, 3 * width), BF)]
    args, scratch, params, kernel = (qkv, qkv, qkv, do), [], {}, attn_bwd_kernel
    if carried is not None:
        h2 = h2.reshape(tokens // seq, 2, seq // 2, width)
        args = args + (carried, h2)
        kernel = attn_carry_kernel
        in_specs = in_specs + [pl.BlockSpec(memory_space=pl.ANY)] * 2
        shapes = ((8, 2048), (32, 512), (8, 1536), (8, 512))
        out_specs = out_specs + [whole(s) for s in shapes] + [pl.BlockSpec(memory_space=pl.ANY)]
        out_shape = out_shape + [jax.ShapeDtypeStruct(s, F32) for s in shapes] + [jax.ShapeDtypeStruct((2 * h2.shape[0],) + h2.shape[2:], BF)]
        scratch = [VMEM(s, F32) for s in (carried.shape,) + shapes] + PHASE_SCRATCH[1] + PHASE_SCRATCH[2] + [DMA] + PHASE_SEMS(2) + FINAL_SEMS + [DMA((3,))]
        params = dict(collective_id=3, has_side_effects=True, vmem_limit_bytes=50 << 20)
    return pl.pallas_call(
        functools.partial(kernel, scale, width),
        grid=(tokens // seq, steps), in_specs=in_specs, out_specs=out_specs, out_shape=out_shape, scratch_shapes=scratch,
        compiler_params=pltpu.CompilerParams(**params),
        name="attn_bwd" if carried is None else "attn_bwd_carry",
    )(*args)


def layer_forward(hidden, first, tokens, weights, layer, seq, scale):
    w_qkv, w_proj, w_up, w_down = weights
    normed, qkv = pre_attn(hidden, first, tokens, w_qkv, layer, seq)
    attn = attn_fwd(qkv, seq, scale)
    mid, normed2, up, gelu, out = post_attn(hidden, first, attn, w_proj, w_up, w_down, layer, seq)
    return out, (hidden, normed, qkv, attn, mid, normed2, up, gelu)


def layer_backward(saved, ct_out, first, weights, layer, seq, scale, carried, h2):
    w_qkv, w_proj, w_up, w_down = weights
    hidden, normed, qkv, attn, mid, normed2, up, gelu = saved
    res = ffn_bwd(gelu, up, ct_out, first, normed2, mid, attn, w_down, w_up, w_proj, layer, seq, carried)
    g_down, g_up, g_proj, ct_mid, ct_attn = res[:5]
    res = attn_bwd(qkv, ct_attn, seq, scale, res[5] if carried is not None else None, h2)
    ct_qkv = res[0]
    g_qkv = dot_tn(normed, ct_qkv)
    grads = (g_qkv, g_proj, g_up, g_down)
    if carried is not None:
        return grads, (res[3], res[4], res[1], res[2]), res[5]
    ct_norm = dot_nt(ct_qkv, w_qkv[layer]).astype(BF)
    ct_hidden = (ct_mid.astype(F32) + rms_pull(hidden.astype(F32), ct_norm.astype(F32))).astype(BF)
    return grads, ct_hidden


def solution(mesh):
    grid = Mesh(mesh.devices.reshape(2, 4, 4, 4), ("pp", "z", "y", "x"))
    dp = ("z", "y", "x")

    def device_step(act_in, loss_seed, w_qkv, w_proj, w_up, w_down):
        micro, _, seq, d = act_in.shape
        mine = micro // 2
        pp = lax.axis_index('pp')
        heads3, hd = w_qkv.shape[2:]
        scale = hd ** -0.5

        full = gather_weights(*(w.reshape(w.shape[1], -1) for w in (w_qkv, w_proj, w_up, w_down)))
        tokens = mine * seq
        act, seed = act_in.reshape(micro * seq, d), loss_seed.reshape(micro * seq, d)
        pp_vec, none = jnp.full((1,), pp, jnp.int32), jnp.zeros((1,), jnp.int32)
        h1, saved0 = layer_forward(act, pp_vec * mine, tokens, full, 0, seq, scale)
        h2, saved1 = layer_forward(h1, none, tokens, full, 1, seq, scale)

        grads1, ct1 = layer_backward(saved1, seed, pp_vec, full, 1, seq, scale, None, None)
        grads0, red1, act_out = layer_backward(saved0, ct1, None, full, 0, seq, scale, grads1, h2)
        act_out = act_out.reshape(micro, 1, seq // 2, d)
        red0 = reduce_grads(grads0, 0)
        outs = [jnp.where(pp == 0, a, b) for a, b in zip(red0, red1)]
        return tuple(o.reshape(w.shape) for o, w in zip(outs, (w_qkv, w_proj, w_up, w_down))) + (act_out,)

    weight_spec = P('pp', dp)
    act_spec = P(None, dp)
    return jax.shard_map(device_step, mesh=grid, in_specs=(act_spec, act_spec) + (weight_spec,) * 4, out_specs=(weight_spec,) * 4 + (P(None, dp, 'pp'),), check_vma=False)
```
